256 devices in a mesh: lat: 16 (over y, x_lo, core), lon: 16 (over z, x_hi).
Axes of the slice: x: 4 (x_hi: 2, x_lo: 2; x = x_hi * 2 + x_lo), y: 4, z: 8, core: 2. Of those that a mesh axis runs over, the one named last changes fastest.
Arguments:
- adjoint: float32 [8, 8, 512, 2048], P(None, None, 'lat', 'lon'), may hold values from -6 to 6
- transport: float32 [6, 8, 512, 2048], P(None, None, 'lat', 'lon'), may hold values from 0.03 to 0.14
- cell_weight: float32 [512, 2048], P('lat', 'lon'), may hold values from 0.1 to 1
- region_local: int32 [512, 2048], P('lat', 'lon'), may hold values from 0 to 255
- tile_regions: int32 [256, 256], replicated, may hold values from 0 to 16383, as said below
- polar_rows: int32 [512], P('lat'), may hold values 0 or 1
- week_index: int32 [1], replicated, may hold values from 0 to 51
- grad_in: bfloat16 [16384, 416], P(('lat', 'lon')), may hold values from -6 to 6
- covariance: bfloat16 [16384, 16384], P(('lat', 'lon')), may hold values from -0.1875 to 0.1875
Outputs:
- adjoint_out: float32 [8, 8, 512, 2048], P(None, None, 'lat', 'lon')
- precond: float32 [16384, 416], P(('lat', 'lon'))
The draws below stay inside these ranges and needn't reach their ends.
Inputs may be any that keep to these rules, and one draw needn't show every extreme that they name: `tile_regions`: each row holds 256 different region numbers; with per = 1, entries o * per to o * per + per - 1 of a row lie in regions o * 64 to o * 64 + 63, for every o.
All inputs are finite; a program needn't handle non-finite values. No bound on the sum of `polar_rows` on one device may be relied on, other than what follows from the above.
Results may differ from the reference program's by a relative error of at most 0.00066.
Values may be sent and summed in bfloat16 or wider, within the bound.
A program may use at most 128 MiB of HBM per device.

```python
import math
import jax
import jax.numpy as jnp

TRC = 8
LEV = 8
CLAT = 32
CLON = 128
LOCAL = 256
REG_DEV = 64
WEEKS = 52
NLAT = 512
NLON = 2048
TILES = 256
REGIONS = 16384
N_LON = 16


def draw_tile_regions(key, part):
    per_owner = LOCAL // TILES
    scores = jax.random.randint(jax.random.fold_in(key, 11), (TILES, TILES, REG_DEV), 0, 1048576, dtype=jnp.int32)
    scores = scores * REG_DEV + jnp.arange(REG_DEV, dtype=jnp.int32)[None, None, :]
    picked = jnp.argsort(scores, axis=2, stable=True)[:, :, :per_owner].astype(jnp.int32)
    offsets = (jnp.arange(TILES, dtype=jnp.int32) * REG_DEV)[None, :, None]
    return (picked + offsets).reshape(TILES, LOCAL).astype(jnp.int32)


def plant(result, rng, smallest, top_value):
    index_at = [jax.random.randint(jax.random.fold_in(rng, axis), (), 0, length) for axis, length in enumerate(result.shape)]
    widest = result.shape.index(max(result.shape))
    next_to = index_at[:widest] + [(index_at[widest] + 1) % result.shape[widest]] + index_at[widest + 1:]
    return result.at[tuple(index_at)].set(smallest).at[tuple(next_to)].set(top_value)


def spiked(values, rng, source, target, blocks, factor):
    owner, partner = [(jnp.arange(values.shape[axis_at]) // (values.shape[axis_at] // blocks)).reshape([-1 if axis == axis_at else 1 for axis in range(values.ndim)]) for axis_at in (source, target)]
    chosen = jax.random.permutation(rng, blocks)[partner]
    strong = (owner == chosen) | (owner == (partner + blocks // 2) % blocks)
    return jnp.where(strong, factor * values, values)


def block_levels(stream_key, extent, pieces, low, top_value):
    def one(position, blocks):
        draws = jax.random.uniform(jax.random.fold_in(jax.random.fold_in(stream_key, 6), position), (blocks,), jnp.float32, low / len(pieces), top_value / len(pieces))
        return jnp.repeat(jnp.exp(draws), extent[position] // blocks).reshape((-1,) + (1,) * (len(extent) - position - 1))

    level = one(*pieces[0])
    for cut in pieces[1:]:
        level = level * one(*cut)
    return level


def gaussian(rng, shape, spread, bound, split=(), kind=jnp.bfloat16):
    drawn = jax.random.normal(rng, shape, jnp.float32) * spread
    if len(split) > 0:
        drawn = block_levels(rng, shape, split, -0.22, 0.18) * drawn
    return jnp.clip(drawn, min=-bound, max=bound).astype(kind)


def bell_draw_with(own_key, shape, deviation, bound, pieces, heavy, kind=jnp.bfloat16):
    drawn = deviation * jax.random.normal(own_key, shape, jnp.float32)
    if pieces:
        drawn = drawn * block_levels(own_key, shape, pieces, -0.22, 0.18)
    return jnp.clip(spiked(drawn, jax.random.fold_in(own_key, 3), *heavy), -bound, bound).astype(kind)


def setup_inputs(seed: int = 0) -> dict:
    key_list = jax.random.split(jax.random.key(seed), 10)
    return {
        "adjoint": gaussian(key_list[0], (TRC, LEV, NLAT, NLON), 1.0, 6.0, ((2, 16), (3, 16)), jnp.float32),
        "transport": jnp.clip(0.03 + 0.11 * jax.random.uniform(key_list[1], (6, LEV, NLAT, NLON), jnp.float32) ** block_levels(key_list[1], (6, LEV, NLAT, NLON), ((2, 16), (3, 16)), -0.2, 0.2), 0.03, 0.14),
        "cell_weight": jnp.clip(jnp.exp(math.log(1.0) - 2.3025851 * jax.random.uniform(key_list[2], (NLAT, NLON), jnp.float32) ** block_levels(key_list[2], (NLAT, NLON), ((0, 16), (1, 16)), -0.2, 0.2)), 0.1, 1.0),
        "region_local": plant(jax.random.randint(key_list[3], (NLAT, NLON), 0, LOCAL), jax.random.fold_in(key_list[3], 1), 0, LOCAL - 1).astype(jnp.int32),
        "tile_regions": draw_tile_regions(jax.random.fold_in(key_list[9], 71), 0),
        "polar_rows": plant((jax.random.randint(key_list[5], (NLAT,), 0, 4) < 1).astype(jnp.int32), jax.random.fold_in(key_list[5], 1), 0, 1),
        "week_index": jax.random.randint(key_list[6], (1,), 0, WEEKS).astype(jnp.int32),
        "grad_in": gaussian(key_list[7], (REGIONS, WEEKS * TRC), 1.0, 6.0, ((0, 256),)),
        "covariance": bell_draw_with(key_list[8], (REGIONS, REGIONS), REGIONS ** -0.5, 0.1875, ((0, 256),), (1, 0, 256, 6.0)),
    }


def advance(field, rates):
    wrapped = jnp.concatenate([field[..., -1:], field, field[..., :1]], axis=3)
    padded = jnp.pad(wrapped, ((0, 0), (0, 0), (1, 1), (0, 0)))
    centre = padded[:, :, 1:-1, 1:-1]
    to_east = padded[:, :, 1:-1, 2:] - centre
    to_west = padded[:, :, 1:-1, :-2] - centre
    to_north = padded[:, :, 2:, 1:-1] - centre
    to_south = padded[:, :, :-2, 1:-1] - centre
    flat_zero = jnp.zeros_like(centre[:, :1])
    upper = jnp.concatenate([centre[:, 1:] - centre[:, :-1], flat_zero], axis=1)
    lower = jnp.concatenate([flat_zero, centre[:, :-1] - centre[:, 1:]], axis=1)
    return (centre + rates[0] * to_east + rates[1] * to_west + rates[2] * to_north
            + rates[3] * to_south + rates[4] * upper + rates[5] * lower)


def reference(adjoint, transport, cell_weight, region_local, tile_regions, polar_rows, week_index, grad_in, covariance):
    field = advance(advance(adjoint, transport), transport)
    zonal = jnp.mean(field, axis=3, keepdims=True)
    flags = polar_rows.astype(jnp.float32)[None, None, :, None]
    adjoint_out = field + 0.5 * flags * (zonal - field)
    surface = adjoint_out[:, 0] * cell_weight[None]
    row_ids = jnp.arange(NLAT, dtype=jnp.int32) // CLAT
    col_ids = jnp.arange(NLON, dtype=jnp.int32) // CLON
    tile_ids = row_ids[:, None] * N_LON + col_ids[None, :]
    gid = tile_regions[tile_ids, region_local]
    fresh = jnp.zeros((REGIONS, TRC), jnp.float32).at[gid.reshape(-1)].add(surface.reshape(TRC, -1).T)
    fresh = fresh.astype(jnp.bfloat16)
    base = jnp.dot(covariance, grad_in, preferred_element_type=jnp.float32)
    added = jnp.dot(covariance, fresh, preferred_element_type=jnp.float32)
    week_hot = (jnp.arange(WEEKS, dtype=jnp.int32) == week_index[0]).astype(jnp.float32)
    precond = base.reshape(REGIONS, WEEKS, TRC) + week_hot[None, :, None] * added[:, None, :]
    return adjoint_out, precond.reshape(REGIONS, WEEKS * TRC)
```

```python
import functools

import jax
import jax.numpy as jnp
from jax import lax
from jax.experimental import pallas as pl
from jax.experimental.pallas import tpu as pltpu
from jax.sharding import PartitionSpec as P

MESH = pl.DeviceIdType.MESH
F32 = jnp.float32
BF16 = jnp.bfloat16
ALL = slice(None)


def dot(a, b):
    return lax.dot_general(a, b, (((1,), (0,)), ((), ())), preferred_element_type=F32)


def dot_nt(a, b):
    return lax.dot_general(a, b, (((1,), (1,)), ((), ())), preferred_element_type=F32)


def kernel(
    adj, tr, weight, rl, flag, reg, grad, week, cov,
    aout, pre,
    first, surf, b0, b1, b2, cmat, fr, col_s, row_n, row_s, col_e, col_w, halo_n, halo_s,
    zbuf, mbuf, xbuf, ybuf, obuf, pacc, precv, aacc, arecv,
    ssem, rsem, lsem,
):
    lat = lax.axis_index("lat")
    lon = lax.axis_index("lon")
    core = lax.rem(lat, 2)
    xl = lax.rem(lat // 2, 2)
    y = lat // 4
    z = lon // 2
    xh = lax.rem(lon, 2)
    x = xh * 2 + xl
    me = {"x": x, "y": y, "z": z}
    size = {"x": 4, "y": 4, "z": 8}
    counter = [0]
    sends = []

    def wrap(v, n):
        return lax.rem(v + 2 * n, n)

    def device(c, at_core):
        return ((c["y"] * 2 + lax.rem(c["x"], 2)) * 2 + at_core, c["z"] * 2 + c["x"] // 2)

    def remote(src, dst, to, k):
        return pltpu.make_async_remote_copy(
            src_ref=src, dst_ref=dst, send_sem=ssem.at[k], recv_sem=rsem.at[k],
            device_id=to, device_id_type=MESH,
        )

    def send(src, dst, to, k):
        c = remote(src, dst, to, k)
        c.start()
        sends.append(c)

    def take(count=1):
        k = counter[0]
        counter[0] += count
        return k

    def arrived(dst, k):
        remote(dst, dst, (lat, lon), k).wait_recv()

    other = (lat + 1 - 2 * core, lon)

    barrier = pltpu.get_barrier_semaphore()
    for k in range(1, 16):
        pl.semaphore_signal(barrier, inc=1, device_id=(lat, wrap(lon + k, 16)), device_id_type=MESH)
        pl.semaphore_signal(barrier, inc=1, device_id=(wrap(lat + k, 16), lon), device_id_type=MESH)
    pl.semaphore_signal(
        barrier, inc=1, device_id=(lat + 2 - 4 * xl, lon + 1 - 2 * xh), device_id_type=MESH
    )

    own_cov = []
    for g in range(8):
        c = pltpu.make_async_copy(
            cov.at[:, pl.ds(pl.multiple_of((g * 2 + core) * 1024, 1024), 1024)],
            cmat.at[g, pl.ds(pl.multiple_of(core * 64, 64), 64), :],
            lsem.at[g],
        )
        c.start()
        own_cov.append(c)

    lane = lax.broadcasted_iota(jnp.int32, (32, 128), 1)
    row = lax.broadcasted_iota(jnp.int32, (32, 128), 0)

    b0[y, xl, z, xh, 0:64, :] = grad[:, 0:128]
    b1[y, xl, z, xh] = grad[:, 128:256]
    b2[y, xl, z, xh] = grad[:, 256:384]
    tail = jnp.zeros((16, 128), F32)
    for q in range(4):
        sel = (
            lax.broadcasted_iota(jnp.int32, (32, 128), 1)
            == lax.broadcasted_iota(jnp.int32, (32, 128), 0) + 32 * q
        ).astype(F32).astype(BF16)
        tail = tail + dot(grad[16 * q:16 * q + 16, 384:416], sel)
    b0[y, xl, z, xh, 64:80, :] = tail.astype(BF16)

    def edges(step, j, v, acc):
        row_n[step, pl.ds(j, 1), :] = v[31:32, :]
        row_s[step, pl.ds(j, 1), :] = v[0:1, :]
        acc = jnp.where(lane == j, pltpu.roll(v, lax.rem(j + 1, 128), 1), acc)
        return jnp.where(lane == j + 64, pltpu.roll(v, j + 64, 1), acc)

    def pack(j, acc):
        return edges(0, j, adj[j], acc)

    col_s[0] = lax.fori_loop(0, 64, pack, jnp.zeros((32, 128), F32), unroll=4)

    pl.semaphore_wait(barrier, 31)

    east, west = wrap(lon + 1, 16), wrap(lon - 1, 16)
    north, south = wrap(lat + 1, 16), wrap(lat - 1, 16)

    def halo_send(s):
        k = take(4)
        send(col_s.at[s], col_w.at[s], (lat, east), k)
        send(col_s.at[s], col_e.at[s], (lat, west), k + 1)
        send(row_n.at[s], halo_s.at[s], (north, lon), k + 2)
        send(row_s.at[s], halo_n.at[s], (south, lon), k + 3)
        return k

    def halo_wait(s, k):
        arrived(col_w.at[s], k)
        arrived(col_e.at[s], k + 1)
        arrived(halo_s.at[s], k + 2)
        arrived(halo_n.at[s], k + 3)

    parts = {
        "a": (b0, "zyx", 48),
        "b": (b1, "yxz", 32),
        "c": (b2, "zxy", 32),
    }

    def slot(buf, at, rows):
        yi = at["y"] if at["y"] is not None else ALL
        zi = at["z"] if at["z"] is not None else ALL
        if at["x"] is None:
            return buf.at[yi, :, zi, :, rows]
        return buf.at[yi, lax.rem(at["x"], 2), zi, at["x"] // 2, rows]

    def whole(buf):
        return pl.ds(0, buf.shape[4])

    ids = {}

    def direct_start(p):
        buf, order, _ = parts[p]
        d = order[0]
        n = size[d]
        k = take(n - 1)
        ids[p, 1] = k
        for i in range(1, n):
            to = dict(me)
            to[d] = wrap(me[d] + i, n)
            here = slot(buf, me, whole(buf))
            send(here, here, device(to, core), k + i - 1)

    def direct_wait(p):
        buf, order, _ = parts[p]
        d = order[0]
        n = size[d]
        for i in range(1, n):
            at = dict(me)
            at[d] = wrap(me[d] - i, n)
            arrived(slot(buf, at, whole(buf)), ids[p, 1] + i - 1)

    def ring(p, stage, s):
        buf, order, half = parts[p]
        d = order[stage - 1]
        n = size[d]
        at = {c: (None if c in order[:stage - 1] else me[c]) for c in "xyz"}
        last = s == n // 2
        rows_r = pl.ds(0, half) if last else whole(buf)
        rows_l = pl.ds(half, buf.shape[4] - half) if last else whole(buf)
        return buf, d, n, at, rows_r, rows_l

    def ring_start(p, stage, s):
        buf, d, n, at, rows_r, rows_l = ring(p, stage, s)
        k = take(2)
        ids[p, stage, s] = k
        right, left = dict(me), dict(me)
        right[d] = wrap(me[d] + 1, n)
        left[d] = wrap(me[d] - 1, n)
        fwd, back = dict(at), dict(at)
        fwd[d] = wrap(me[d] - (s - 1), n)
        back[d] = wrap(me[d] + (s - 1), n)
        src = slot(buf, fwd, rows_r)
        send(src, src, device(right, core), k)
        src = slot(buf, back, rows_l)
        send(src, src, device(left, core), k + 1)

    def ring_wait(p, stage, s):
        buf, d, n, at, rows_r, rows_l = ring(p, stage, s)
        k = ids[p, stage, s]
        fwd, back = dict(at), dict(at)
        fwd[d] = wrap(me[d] - s, n)
        back[d] = wrap(me[d] + s, n)
        arrived(slot(buf, fwd, rows_r), k)
        arrived(slot(buf, back, rows_l), k + 1)

    plan = {}
    for p, (_, order, _) in parts.items():
        steps = [(stage, s) for stage in (2, 3) for s in range(1, size[order[stage - 1]] // 2 + 1)]
        plan[p] = steps

    def pump(p, i):
        steps = plan[p]
        if i == 1:
            direct_wait(p)
        else:
            ring_wait(p, *steps[i - 2])
        if i <= len(steps):
            ring_start(p, *steps[i - 1])

    k1 = halo_send(0)
    for p in "bac":
        direct_start(p)
    k_cov = take(8)
    for g in range(8):
        send(
            cov.at[:, pl.ds(pl.multiple_of((g * 2 + 1 - core) * 1024, 1024), 1024)],
            cmat.at[g, pl.ds(pl.multiple_of(core * 64, 64), 64), :],
            other, k_cov + g,
        )

    has_north = (lat < 15).astype(F32)
    has_south = (lat > 0).astype(F32)

    def stencil(src, step, j):
        l = lax.rem(j, 8)
        c = src[j]
        ce = col_e[step]
        cw = col_w[step]
        e = pltpu.roll(jnp.where(lane == 0, pltpu.roll(ce, 64 - j, 1), c), 127, 1)
        v = pltpu.roll(jnp.where(lane == 127, pltpu.roll(cw, 127 - j, 1), c), 1, 1)
        n = jnp.where(row == 31, has_north * halo_n[step, pl.ds(j, 1), :], pltpu.roll(c, 31, 0))
        s = jnp.where(row == 0, has_south * halo_s[step, pl.ds(j, 1), :], pltpu.roll(c, 1, 0))
        u = src[j + jnp.minimum(7 - l, 1)]
        d = src[j - jnp.minimum(l, 1)]
        return (
            c + tr[l] * (e - c) + tr[8 + l] * (v - c) + tr[16 + l] * (n - c)
            + tr[24 + l] * (s - c) + tr[32 + l] * (u - c) + tr[40 + l] * (d - c)
        )

    halo_wait(0, k1)

    def step_one(j, acc):
        v = stencil(adj, 0, j)
        first[j] = v
        return edges(1, j, v, acc)

    col_s[1] = lax.fori_loop(0, 64, step_one, jnp.zeros((32, 128), F32), unroll=2)
    k2 = halo_send(1)
    pump("b", 1)
    pump("a", 1)
    pump("c", 1)
    halo_wait(1, k2)

    def step_two(j, acc):
        v = stencil(first, 1, j)
        aout[j] = v
        return jnp.where(lane == j, jnp.sum(v, axis=1, keepdims=True), acc)

    sums = lax.fori_loop(0, 64, step_two, jnp.zeros((32, 128), F32), unroll=2)
    lane16 = lax.broadcasted_iota(jnp.int32, (16, 128), 1)
    row16 = lax.broadcasted_iota(jnp.int32, (16, 128), 0)
    zbuf[lon] = jnp.where(lane16 < 64, sums[0:16], pltpu.roll(sums[16:32], 64, 1))
    kz = take(15)
    for i in range(1, 16):
        send(zbuf.at[lon], zbuf.at[lon], (lat, wrap(lon + i, 16)), kz + i - 1)
    pump("b", 2)
    pump("a", 2)
    pump("c", 2)
    pump("b", 3)
    for i in range(1, 16):
        arrived(zbuf.at[wrap(lon - i, 16)], kz + i - 1)
    total = zbuf[0]
    for i in range(1, 16):
        total = total + zbuf[i]
    total = total * (1.0 / 2048.0)
    mean = jnp.concatenate([total, pltpu.roll(total, 64, 1)], axis=0)
    flags = 0.5 * flag[...]

    def filtered(j):
        v = aout[j]
        return v + flags * (jnp.sum(jnp.where(lane == j, mean, 0.0), axis=1, keepdims=True) - v)

    for t in range(8):
        surf[t] = filtered(8 * t) * weight[...]

    pump("a", 3)
    pump("c", 3)

    sub8 = lax.broadcasted_iota(jnp.int32, (16, 128), 0)

    def regions(r, acc):
        lhs, rhs = [], [[], [], []]
        for h in range(2):
            i = 2 * r + h
            local = rl[pl.ds(i, 1), :]
            low = jnp.broadcast_to(local & 15, (16, 128))
            high = jnp.broadcast_to(local >> 4, (8, 128))
            lhs.append((low == sub8).astype(F32).astype(BF16))
            s = jnp.concatenate([surf[t, pl.ds(i, 1), :] for t in range(8)], axis=0)
            for n in range(3):
                piece = s.astype(BF16).astype(F32)
                s = s - piece
                rhs[n].append(
                    jnp.concatenate([jnp.where(high == a, piece, 0.0) for a in range(16)], axis=0).astype(BF16)
                )
        left = jnp.concatenate(lhs, axis=1)
        for n in range(3):
            acc = acc + dot_nt(left, jnp.concatenate(rhs[n], axis=1))
        return acc

    m = lax.fori_loop(0, 16, regions, jnp.zeros((16, 128), F32))
    for i in range(16):
        mbuf[i] = m[i:i + 1, :]
    xbuf[lon] = mbuf[lon]
    kx = take(15)
    for i in range(1, 16):
        to = wrap(lon + i, 16)
        send(mbuf.at[to], xbuf.at[lon], (lat, to), kx + i - 1)

    def rest(j, carry):
        aout[j] = filtered(j)
        return carry

    lax.fori_loop(0, 64, rest, 0, unroll=2)
    pump("b", 4)
    for i in range(1, 16):
        arrived(xbuf.at[wrap(lon - i, 16)], kx + i - 1)
    got = jnp.concatenate([xbuf[i] for i in range(16)], axis=0)
    turned = jnp.zeros((16, 128), F32)
    group = lane16 // 8
    for d in range(16):
        moved = got if d == 0 else pltpu.roll(pltpu.roll(got, 16 - d, 0), 8 * d, 1)
        turned = jnp.where(lax.rem(group - row16 + 16, 16) == d, moved, turned)
    for i in range(16):
        ybuf[i] = turned[i:i + 1, :]
    obuf[lat] = ybuf[lat]
    ky = take(15)
    for i in range(1, 16):
        to = wrap(lat + i, 16)
        send(ybuf.at[to], obuf.at[lat], (to, lon), ky + i - 1)
    pump("b", 5)
    for i in range(1, 16):
        arrived(obuf.at[wrap(lat - i, 16)], ky + i - 1)

    lane8 = lax.broadcasted_iota(jnp.int32, (8, 128), 1)
    row8 = lax.broadcasted_iota(jnp.int32, (8, 128), 0)
    packed = jnp.zeros((8, 128), F32)
    for v in range(8):
        f = jnp.zeros((8, 128), F32)
        for a in range(16):
            f = f + jnp.where(reg[a:a + 1, :] == row8 + 8 * v, obuf[a], 0.0)
        for shift in (64, 32, 16, 8):
            f = f + pltpu.roll(f, shift, 1)
        packed = jnp.where(lane8 // 8 == v, f, packed)
    fr[y, xl, z, xh] = packed.astype(BF16).astype(F32)
    kf = take(15)
    for i in range(1, 16):
        here = fr.at[y, xl, z, xh]
        send(here, here, (lat, wrap(lon + i, 16)), kf + i - 1)
    pump("a", 4)
    pump("c", 4)
    for i in range(1, 16):
        o = wrap(lon - i, 16)
        arrived(fr.at[y, xl, o // 2, lax.rem(o, 2)], kf + i - 1)
    kg = take(7)
    for i in range(1, 8):
        g = wrap(lat // 2 + i, 8)
        send(fr.at[y, xl], fr.at[y, xl], (g * 2 + core, lon), kg + i - 1)
    pump("b", 6)
    pump("a", 5)
    pump("c", 5)
    pump("b", 7)
    for c in own_cov:
        c.wait()
    for g in range(8):
        arrived(cmat.at[g, pl.ds(pl.multiple_of((1 - core) * 64, 64), 64), :], k_cov + g)

    pacc[...] = jnp.zeros((2, 64, 512), F32)

    def product(g, carry):
        gy, gx = g // 2, lax.rem(g, 2)
        c = cmat[g]
        r0 = jnp.concatenate(
            [b0[gy, gx][:, :, 0:64].reshape(1024, 128), b1[gy, gx].reshape(1024, 128)], axis=1
        )
        left = dot(c, r0)
        pacc[0, :, 0:256] += left[0:64]
        pacc[1, :, 0:256] += left[64:128]
        tails = b0[gy, gx][:, :, 64:80].reshape(256, 128)
        pieces = []
        for q in range(4):
            sel = (
                lax.broadcasted_iota(jnp.int32, (128, 128), 0)
                == lax.broadcasted_iota(jnp.int32, (128, 128), 1) + 32 * q
            ).astype(F32).astype(BF16)
            pieces.append(dot(tails, sel).astype(BF16).reshape(16, 16, 128))
        last = jnp.concatenate(pieces, axis=1).reshape(1024, 128)
        right = dot(c, jnp.concatenate([b2[gy, gx].reshape(1024, 128), last], axis=1))
        pacc[0, :, 256:512] += right[0:64]
        pacc[1, :, 256:512] += right[64:128]
        return carry

    lax.fori_loop(0, 8, product, 0)
    kp = take()
    send(pacc.at[1 - core], precv, other, kp)

    for i in range(1, 8):
        g = wrap(lat // 2 - i, 8)
        arrived(fr.at[g // 2, lax.rem(g, 2)], kg + i - 1)

    def fresh_product(g, acc):
        f = fr[g // 2, lax.rem(g, 2)].reshape(16, 8, 128)
        lanes = lax.broadcasted_iota(jnp.int32, (16, 8, 128), 2) // 8
        w = jnp.concatenate([jnp.where(lanes == v, f, 0.0) for v in range(8)], axis=1)
        return acc + dot(cmat[g], w.astype(BF16).reshape(1024, 128))

    added = lax.fori_loop(0, 8, fresh_product, jnp.zeros((128, 128), F32))
    for shift in (64, 32, 16, 8):
        added = added + pltpu.roll(added, shift, 1)
    aacc[0] = added[0:64]
    aacc[1] = added[64:128]
    ka = take()
    send(aacc.at[1 - core], arecv, other, ka)
    arrived(precv, kp)
    arrived(arecv, ka)
    mine = aacc[core] + arecv[...]
    base = pacc[core] + precv[...]
    for n in range(4):
        week_of = (lax.broadcasted_iota(jnp.int32, (64, 128), 1) + 128 * n) // 8
        pre[:, 128 * n:128 * n + 128] = base[:, 128 * n:128 * n + 128] + jnp.where(
            week_of == week[...], mine, 0.0
        )
    for c in sends:
        c.wait_send()


COPIES = 160


def shards(adjoint, transport, cell_weight, region_local, tile_regions, polar_rows, week_index, grad_in, covariance):
    me = lax.axis_index("lat") * 16 + lax.axis_index("lon")
    flag = jnp.broadcast_to(polar_rows.astype(F32)[:, None], (32, 128))
    owned = lax.dynamic_slice_in_dim(tile_regions, me, 1, axis=1).reshape(16, 16) - me * 64
    reg = jnp.broadcast_to(owned[:, :, None], (16, 16, 8)).reshape(16, 128)
    week = jnp.broadcast_to(week_index.reshape(1, 1), (64, 128))
    vmem = pl.BlockSpec(memory_space=pltpu.VMEM)
    aout, pre = pl.pallas_call(
        kernel,
        out_shape=(
            jax.ShapeDtypeStruct((64, 32, 128), F32),
            jax.ShapeDtypeStruct((64, 512), F32),
        ),
        in_specs=[vmem] * 8 + [pl.BlockSpec(memory_space=pl.ANY)],
        out_specs=(vmem, vmem),
        scratch_shapes=[
            pltpu.VMEM((64, 32, 128), F32),
            pltpu.VMEM((8, 32, 128), F32),
            pltpu.VMEM((4, 2, 8, 2, 80, 128), BF16),
            pltpu.VMEM((4, 2, 8, 2, 64, 128), BF16),
            pltpu.VMEM((4, 2, 8, 2, 64, 128), BF16),
            pltpu.VMEM((8, 128, 1024), BF16),
            pltpu.VMEM((4, 2, 8, 2, 8, 128), F32),
            pltpu.VMEM((2, 32, 128), F32),
            pltpu.VMEM((2, 64, 128), F32),
            pltpu.VMEM((2, 64, 128), F32),
            pltpu.VMEM((2, 32, 128), F32),
            pltpu.VMEM((2, 32, 128), F32),
            pltpu.VMEM((2, 64, 128), F32),
            pltpu.VMEM((2, 64, 128), F32),
            pltpu.VMEM((16, 16, 128), F32),
            pltpu.VMEM((16, 1, 128), F32),
            pltpu.VMEM((16, 1, 128), F32),
            pltpu.VMEM((16, 1, 128), F32),
            pltpu.VMEM((16, 1, 128), F32),
            pltpu.VMEM((2, 64, 512), F32),
            pltpu.VMEM((64, 512), F32),
            pltpu.VMEM((2, 64, 128), F32),
            pltpu.VMEM((64, 128), F32),
            pltpu.SemaphoreType.DMA((COPIES,)),
            pltpu.SemaphoreType.DMA((COPIES,)),
            pltpu.SemaphoreType.DMA((8,)),
        ],
        compiler_params=pltpu.CompilerParams(
            collective_id=0, has_side_effects=True, vmem_limit_bytes=40 * 1024 * 1024
        ),
        name="window",
    )(
        adjoint.reshape(64, 32, 128),
        transport.reshape(48, 32, 128),
        cell_weight, region_local, flag, reg, grad_in, week, covariance,
    )
    return aout.reshape(8, 8, 32, 128), pre[:, :416]


def solution(mesh):
    both = ("lat", "lon")
    return jax.shard_map(
        shards,
        mesh=mesh,
        in_specs=(
            P(None, None, "lat", "lon"), P(None, None, "lat", "lon"), P("lat", "lon"), P("lat", "lon"),
            P(), P("lat"), P(), P(both, None), P(both, None),
        ),
        out_specs=(P(None, None, "lat", "lon"), P(both, None)),
        check_vma=False,
    )
```

```python
import functools

import jax
import jax.numpy as jnp
from jax import lax
from jax.experimental import pallas as pl
from jax.experimental.pallas import tpu as pltpu
from jax.sharding import PartitionSpec as P

MESH = pl.DeviceIdType.MESH
F32 = jnp.float32
BF16 = jnp.bfloat16
ALL = slice(None)


def dot(a, b):
    return lax.dot_general(a, b, (((1,), (0,)), ((), ())), preferred_element_type=F32)


def dot_nt(a, b):
    return lax.dot_general(a, b, (((1,), (1,)), ((), ())), preferred_element_type=F32)


def kernel(
    adj_h, tr_h, weight_h, rl_h, tiles_h, polar_h, week_h, grad, cov,
    aout_h, pre_h,
    adj, tr, weight, rl, tiles, polar, week, gtail,
    first, surf, b0, b1, b2, cmat, fr, col_s, row_n, row_s, col_e, col_w, halo_n, halo_s,
    zbuf, ybar, mbuf, xbuf, ybuf, obuf, pacc, precv, aacc, arecv,
    aout, pre, ssem, rsem, lsem, insem,
):
    lat = lax.axis_index("lat")
    lon = lax.axis_index("lon")
    core = lax.rem(lat, 2)
    xl = lax.rem(lat // 2, 2)
    y = lat // 4
    z = lon // 2
    xh = lax.rem(lon, 2)
    x = xh * 2 + xl
    me = {"x": x, "y": y, "z": z}
    size = {"x": 4, "y": 4, "z": 8}
    counter = [0]
    sends = []

    def wrap(v, n):
        return lax.rem(v + 2 * n, n)

    def device(c, at_core):
        return ((c["y"] * 2 + lax.rem(c["x"], 2)) * 2 + at_core, c["z"] * 2 + c["x"] // 2)

    def remote(src, dst, to, k):
        return pltpu.make_async_remote_copy(
            src_ref=src, dst_ref=dst, send_sem=ssem.at[k], recv_sem=rsem.at[k],
            device_id=to, device_id_type=MESH,
        )

    def send(src, dst, to, k):
        c = remote(src, dst, to, k)
        c.start()
        sends.append(c)

    def take(count=1):
        k = counter[0]
        counter[0] += count
        return k

    def arrived(dst, k):
        remote(dst, dst, (lat, lon), k).wait_recv()

    other = (lat + 1 - 2 * core, lon)

    cur = [None]

    def mark(n):
        if PROFILE:
            if cur[0] is not None:
                cur[0].__exit__(None, None, None)
            cur[0] = jax.named_scope(n) if n else None
            if n:
                cur[0].__enter__()

    mark("s00_entry")
    barrier = pltpu.get_barrier_semaphore()
    for k in range(1, 16):
        pl.semaphore_signal(barrier, inc=1, device_id=(lat, wrap(lon + k, 16)), device_id_type=MESH)
        pl.semaphore_signal(barrier, inc=1, device_id=(wrap(lat + k, 16), lon), device_id_type=MESH)
    pl.semaphore_signal(
        barrier, inc=1, device_id=(lat + 2 - 4 * xl, lon + 1 - 2 * xh), device_id_type=MESH
    )

    def load(src, dst, k):
        c = pltpu.make_async_copy(src, dst, insem.at[k])
        c.start()
        return c

    in_adj = [load(adj_h.at[:, l], adj.at[l], l) for l in range(8)]
    in_grad = [
        load(grad.at[:, 0:128], b0.at[y, xl, z, xh, 0:64], 8),
        load(grad.at[:, 128:256], b1.at[y, xl, z, xh], 9),
        load(grad.at[:, 256:384], b2.at[y, xl, z, xh], 10),
        load(grad, gtail, 11),
    ]
    in_tr = load(tr_h, tr, 12)
    number = lat * 16 + lon
    lanes_at = pl.multiple_of(number // 128 * 128, 128)
    in_late = [
        load(weight_h, weight, 13), load(rl_h, rl, 14), load(polar_h, polar, 15),
        load(tiles_h.at[:, pl.ds(lanes_at, 128)], tiles, 16), load(week_h, week, 17),
    ]
    own_cov = []
    for g in range(8):
        c = pltpu.make_async_copy(
            cov.at[:, pl.ds(pl.multiple_of((g * 2 + core) * 1024, 1024), 1024)],
            cmat.at[g, pl.ds(pl.multiple_of(core * 64, 64), 64), :],
            lsem.at[g],
        )
        c.start()
        own_cov.append(c)

    lane = lax.broadcasted_iota(jnp.int32, (32, 128), 1)
    row = lax.broadcasted_iota(jnp.int32, (32, 128), 0)

    def edges(step, j, v, acc):
        row_n[step, pl.ds(j, 1), :] = v[31:32, :]
        row_s[step, pl.ds(j, 1), :] = v[0:1, :]
        return jnp.where(lane // 2 == j, pltpu.roll(v, lax.rem(2 * j + 1, 128), 1), acc)

    def pack(j, acc):
        return edges(0, j, adj[j // 8, lax.rem(j, 8)], acc)

    none = jnp.zeros((32, 128), F32)
    in_adj[0].wait()
    in_adj[1].wait()
    col_s[0] = lax.fori_loop(0, 16, pack, none, unroll=4)
    for c in in_adj[2:]:
        c.wait()
    col_s[1] = lax.fori_loop(16, 64, pack, none, unroll=4)

    for c in in_grad:
        c.wait()
    tail = jnp.zeros((16, 128), F32)
    for q in range(4):
        sel = (
            lax.broadcasted_iota(jnp.int32, (32, 128), 1)
            == lax.broadcasted_iota(jnp.int32, (32, 128), 0) + 32 * q
        ).astype(F32).astype(BF16)
        tail = tail + dot(gtail[16 * q:16 * q + 16, 384:416], sel)
    b0[y, xl, z, xh, 64:80, :] = tail.astype(BF16)

    mark("s01_barrier")
    pl.semaphore_wait(barrier, 31)
    mark("s02_send1")

    east, west = wrap(lon + 1, 16), wrap(lon - 1, 16)
    north, south = wrap(lat + 1, 16), wrap(lat - 1, 16)

    def halo_send(s, i, lo, hi):
        k = take(4)
        rows = pl.ds(lo, hi - lo)
        send(row_n.at[s, rows], halo_s.at[s, rows], (north, lon), k + 2)
        send(row_s.at[s, rows], halo_n.at[s, rows], (south, lon), k + 3)
        send(col_s.at[2 * s + i], col_w.at[2 * s + i], (lat, east), k)
        send(col_s.at[2 * s + i], col_e.at[2 * s + i], (lat, west), k + 1)
        return k

    def halo_wait(s, i, lo, hi, k):
        rows = pl.ds(lo, hi - lo)
        arrived(col_w.at[2 * s + i], k)
        arrived(col_e.at[2 * s + i], k + 1)
        arrived(halo_s.at[s, rows], k + 2)
        arrived(halo_n.at[s, rows], k + 3)
        return jnp.where(lax.rem(lane, 2) == 1, col_e[2 * s + i], pltpu.roll(col_w[2 * s + i], 2, 1))

    parts = {
        "a": (b0, "zyx", 48),
        "b": (b1, "yxz", 32),
        "c": (b2, "zxy", 32),
    }

    def slot(buf, at, rows):
        yi = at["y"] if at["y"] is not None else ALL
        zi = at["z"] if at["z"] is not None else ALL
        if at["x"] is None:
            return buf.at[yi, :, zi, :, rows]
        return buf.at[yi, lax.rem(at["x"], 2), zi, at["x"] // 2, rows]

    def whole(buf):
        return pl.ds(0, buf.shape[4])

    ids = {}

    def direct_start(p):
        buf, order, _ = parts[p]
        d = order[0]
        n = size[d]
        k = take(n - 1)
        ids[p, 1] = k
        for i in range(1, n):
            to = dict(me)
            to[d] = wrap(me[d] + i, n)
            here = slot(buf, me, whole(buf))
            send(here, here, device(to, core), k + i - 1)

    def direct_wait(p):
        buf, order, _ = parts[p]
        d = order[0]
        n = size[d]
        for i in range(1, n):
            at = dict(me)
            at[d] = wrap(me[d] - i, n)
            arrived(slot(buf, at, whole(buf)), ids[p, 1] + i - 1)

    groups = ((0,), (1, 3), (2,))

    def ring(p, stage, s, off):
        buf, order, half = parts[p]
        d = order[stage - 1]
        n = size[d]
        at = {c: (None if c in order[:stage - 1] else me[c]) for c in "xyz"}
        if stage == 3:
            at[order[1]] = wrap(me[order[1]] + off, 4)
        last = s == n // 2
        rows_r = pl.ds(0, half) if last else whole(buf)
        rows_l = pl.ds(half, buf.shape[4] - half) if last else whole(buf)
        return buf, d, n, at, rows_r, rows_l

    def ring_start(p, stage, s, g):
        for off in groups[g]:
            buf, d, n, at, rows_r, rows_l = ring(p, stage, s, off)
            k = take(2)
            ids[p, stage, s, off] = k
            right, left = dict(me), dict(me)
            right[d] = wrap(me[d] + 1, n)
            left[d] = wrap(me[d] - 1, n)
            fwd, back = dict(at), dict(at)
            fwd[d] = wrap(me[d] - (s - 1), n)
            back[d] = wrap(me[d] + (s - 1), n)
            src = slot(buf, fwd, rows_r)
            send(src, src, device(right, core), k)
            src = slot(buf, back, rows_l)
            send(src, src, device(left, core), k + 1)

    def ring_wait(p, stage, s, g):
        for off in groups[g]:
            buf, d, n, at, rows_r, rows_l = ring(p, stage, s, off)
            k = ids[p, stage, s, off]
            fwd, back = dict(at), dict(at)
            fwd[d] = wrap(me[d] - s, n)
            back[d] = wrap(me[d] + s, n)
            arrived(slot(buf, fwd, rows_r), k)
            arrived(slot(buf, back, rows_l), k + 1)

    short = (
        ((), ((2, 1, 0), (3, 1, 0))),
        (((2, 1, 0),), ((2, 2, 0), (3, 1, 1))),
        (((3, 1, 0),), ((3, 2, 0),)),
        (((2, 2, 0),), ((3, 1, 2),)),
        (((3, 1, 1),), ((3, 2, 1),)),
        (((3, 1, 2),), ((3, 2, 2),)),
        (((3, 2, 0), (3, 2, 1), (3, 2, 2)), ()),
    )
    long = short[:3] + (
        short[3],
        short[4],
        (((3, 2, 0),), ((3, 3, 0),)),
        (((3, 1, 2),), ((3, 2, 2),)),
        (((3, 2, 1),), ((3, 3, 1),)),
        (((3, 3, 0),), ((3, 4, 0),)),
        (((3, 2, 2),), ((3, 3, 2),)),
        (((3, 3, 1),), ((3, 4, 1),)),
        (((3, 3, 2),), ((3, 4, 2),)),
        (((3, 4, 0), (3, 4, 1), (3, 4, 2)), ()),
    )
    plan = {"a": short, "b": long, "c": short}

    def pump(p, *events):
        for i in events:
            waits, starts = plan[p][i - 1]
            if i == 1:
                direct_wait(p)
            for w in waits:
                ring_wait(p, *w)
            for w in starts:
                ring_start(p, *w)

    k1a = halo_send(0, 0, 0, 16)
    k1b = halo_send(0, 1, 16, 64)
    for p in "bac":
        direct_start(p)
    k_cov = take(8)
    for g in range(8):
        send(
            cov.at[:, pl.ds(pl.multiple_of((g * 2 + 1 - core) * 1024, 1024), 1024)],
            cmat.at[g, pl.ds(pl.multiple_of(core * 64, 64), 64), :],
            other, k_cov + g,
        )

    has_north = (lat < 15).astype(F32)
    has_south = (lat > 0).astype(F32)

    def stencil(src, step, j, sides):
        l, t = j // 8, lax.rem(j, 8)
        c = src[l, t]
        h = pltpu.roll(sides, 126 - 2 * j, 1)
        e = jnp.where(lane == 127, h, pltpu.roll(c, 127, 1))
        v = jnp.where(lane == 0, h, pltpu.roll(c, 1, 1))
        n = jnp.where(row == 31, has_north * halo_n[step, pl.ds(j, 1), :], pltpu.roll(c, 31, 0))
        s = jnp.where(row == 0, has_south * halo_s[step, pl.ds(j, 1), :], pltpu.roll(c, 1, 0))
        u = src[jnp.minimum(l + 1, 7), t]
        d = src[jnp.maximum(l - 1, 0), t]
        return (
            c + tr[0, l] * (e - c) + tr[1, l] * (v - c) + tr[2, l] * (n - c)
            + tr[3, l] * (s - c) + tr[4, l] * (u - c) + tr[5, l] * (d - c)
        )

    mark("s03_halo1a")
    in_tr.wait()
    sides1a = halo_wait(0, 0, 0, 16, k1a)
    mark("s04_step1a")

    def step_one(sides):
        def body(j, acc):
            v = stencil(adj, 0, j, sides)
            first[j // 8, lax.rem(j, 8)] = v
            return edges(1, j, v, acc)
        return body

    col_s[2] = lax.fori_loop(0, 8, step_one(sides1a), none, unroll=UNROLL)
    k2a = halo_send(1, 0, 0, 8)
    mark("s05_step1a2")
    rest1 = lax.fori_loop(8, 16, step_one(sides1a), none, unroll=UNROLL)
    mark("s06_pump")
    pump("b", 1)
    mark("s07_halo1b")
    sides1b = halo_wait(0, 1, 16, 64, k1b)
    mark("s08_step1b")
    col_s[3] = lax.fori_loop(16, 64, step_one(sides1b), rest1, unroll=UNROLL)
    k2b = halo_send(1, 1, 8, 64)
    mark("s09_pump")
    pump("b", 2)
    pump("a", 1)
    pump("c", 1)
    mark("s10_halo2a")
    sides2a = halo_wait(1, 0, 0, 8, k2a)
    mark("s11_step2a")

    def step_two(sides):
        def body(j, acc):
            v = stencil(first, 1, j, sides)
            aout[lax.rem(j, 8), j // 8] = v
            return jnp.where(lane == j, jnp.sum(v, axis=1, keepdims=True), acc)
        return body

    sums = lax.fori_loop(0, 8, step_two(sides2a), none, unroll=UNROLL)
    lane8 = lax.broadcasted_iota(jnp.int32, (8, 128), 1)
    row8 = lax.broadcasted_iota(jnp.int32, (8, 128), 0)
    tight = sums[0:8]
    for i in range(1, 4):
        tight = jnp.where(lane8 // 8 == i, pltpu.roll(sums[8 * i:8 * i + 8], 8 * i, 1), tight)
    ybar[lon] = tight
    kz = take(15)
    for i in range(1, 16):
        send(ybar.at[lon], ybar.at[lon], (lat, wrap(lon + i, 16)), kz + i - 1)
    mark("s12_pump")
    pump("b", 3)
    pump("b", 4)
    mark("s13_halo2b")
    sides2b = halo_wait(1, 1, 8, 64, k2b)
    mark("s14_step2b")
    sums = lax.fori_loop(8, 64, step_two(sides2b), none, unroll=UNROLL)
    lane16 = lax.broadcasted_iota(jnp.int32, (16, 128), 1)
    row16 = lax.broadcasted_iota(jnp.int32, (16, 128), 0)
    zbuf[lon] = jnp.where(lane16 < 64, sums[0:16], pltpu.roll(sums[16:32], 64, 1))
    kw = take(15)
    for i in range(1, 16):
        send(zbuf.at[lon], zbuf.at[lon], (lat, wrap(lon + i, 16)), kw + i - 1)
    mark("s15_pump")
    pump("a", 2)
    pump("c", 2)
    pump("b", 5)
    pump("b", 6)
    for c in in_late:
        c.wait()
    flags = 0.5 * jnp.sum(
        jnp.where(lane == row, jnp.broadcast_to(polar[...], (32, 128)), 0).astype(F32), axis=1, keepdims=True
    )
    lane256 = lax.broadcasted_iota(jnp.int32, (256, 128), 1)
    row256 = lax.broadcasted_iota(jnp.int32, (256, 128), 0)
    mine_at = jnp.sum(
        jnp.where(lane256 == number - lanes_at, tiles[...] - 64 * number, 0).astype(F32), axis=1, keepdims=True
    )
    spread = jnp.where(lane256 // 8 == lax.rem(row256, 16), mine_at, 0.0).astype(BF16)
    pick = (
        lax.broadcasted_iota(jnp.int32, (16, 256), 1) // 16 == lax.broadcasted_iota(jnp.int32, (16, 256), 0)
    ).astype(F32).astype(BF16)
    reg = dot(pick, spread).astype(jnp.int32)
    mark("s16_zwait")
    for i in range(1, 16):
        arrived(ybar.at[wrap(lon - i, 16)], kz + i - 1)
    mark("s17_surf")
    total = ybar[0]
    for i in range(1, 16):
        total = total + ybar[i]
    total = total * (1.0 / 2048.0)
    mean0 = jnp.concatenate([total] + [pltpu.roll(total, 128 - 8 * i, 1) for i in range(1, 4)], axis=0)

    def filtered(j, mean):
        v = aout[lax.rem(j, 8), j // 8]
        v = v + flags * (jnp.sum(jnp.where(lane == j, mean, 0.0), axis=1, keepdims=True) - v)
        aout[lax.rem(j, 8), j // 8] = v
        return v

    for t in range(8):
        surf[t] = filtered(t, mean0) * weight[...]

    mark("s18_pump")
    pump("a", 3)
    pump("c", 3)
    pump("b", 7)
    mark("s19_regions")

    sub8 = lax.broadcasted_iota(jnp.int32, (16, 128), 0)

    def regions(r, acc):
        lhs, rhs = [], [[], [], []]
        for h in range(2):
            i = 2 * r + h
            local = rl[pl.ds(i, 1), :]
            low = jnp.broadcast_to(local & 15, (16, 128))
            high = jnp.broadcast_to(local >> 4, (8, 128))
            lhs.append((low == sub8).astype(F32).astype(BF16))
            s = jnp.concatenate([surf[t, pl.ds(i, 1), :] for t in range(8)], axis=0)
            for n in range(3):
                piece = s.astype(BF16).astype(F32)
                s = s - piece
                rhs[n].append(
                    jnp.concatenate([jnp.where(high == a, piece, 0.0) for a in range(16)], axis=0).astype(BF16)
                )
        left = jnp.concatenate(lhs, axis=1)
        for n in range(3):
            acc = acc + dot_nt(left, jnp.concatenate(rhs[n], axis=1))
        return acc

    m = lax.fori_loop(0, 16, regions, jnp.zeros((16, 128), F32), unroll=2)
    for i in range(16):
        mbuf[i] = m[i:i + 1, :]
    xbuf[lon] = mbuf[lon]
    kx = take(15)
    for i in range(1, 16):
        to = wrap(lon + i, 16)
        send(mbuf.at[to], xbuf.at[lon], (lat, to), kx + i - 1)

    mark("s20_pump")
    pump("a", 4)
    pump("c", 4)
    pump("b", 8)
    pump("b", 9)
    mark("s21_rest")
    for i in range(1, 16):
        arrived(zbuf.at[wrap(lon - i, 16)], kw + i - 1)
    total = zbuf[0]
    for i in range(1, 16):
        total = total + zbuf[i]
    total = total * (1.0 / 2048.0)
    mean = jnp.concatenate([total, pltpu.roll(total, 64, 1)], axis=0)

    def rest(j, carry):
        filtered(j, mean)
        return carry

    lax.fori_loop(8, 64, rest, 0, unroll=UNROLL)
    out_field = load(aout, aout_h, 18)
    mark("s22_pump")
    pump("a", 5)
    pump("c", 5)
    pump("b", 10)
    pump("b", 11)
    mark("s23_xwait")
    for i in range(1, 16):
        arrived(xbuf.at[wrap(lon - i, 16)], kx + i - 1)
    mark("s24_turn")
    got = jnp.concatenate([xbuf[i] for i in range(16)], axis=0)
    turned = jnp.zeros((16, 128), F32)
    group = lane16 // 8
    for d in range(16):
        moved = got if d == 0 else pltpu.roll(pltpu.roll(got, 16 - d, 0), 8 * d, 1)
        turned = jnp.where(lax.rem(group - row16 + 16, 16) == d, moved, turned)
    for i in range(16):
        ybuf[i] = turned[i:i + 1, :]
    obuf[lat] = ybuf[lat]
    ky = take(15)
    for i in range(1, 16):
        to = wrap(lat + i, 16)
        send(ybuf.at[to], obuf.at[lat], (to, lon), ky + i - 1)
    mark("s25_pump")
    pump("a", 6)
    pump("c", 6)
    pump("b", 12)
    mark("s26_owait")
    for i in range(1, 16):
        arrived(obuf.at[wrap(lat - i, 16)], ky + i - 1)

    mark("s27_fresh")
    packed = jnp.zeros((8, 128), F32)
    for v in range(8):
        f = jnp.zeros((8, 128), F32)
        for a in range(16):
            f = f + jnp.where(reg[a:a + 1, :] == row8 + 8 * v, obuf[a], 0.0)
        for shift in (64, 32, 16, 8):
            f = f + pltpu.roll(f, shift, 1)
        packed = jnp.where(lane8 // 8 == v, f, packed)
    fr[y, xl, z, xh] = packed.astype(BF16).astype(F32)
    kf = take(15)
    for i in range(1, 16):
        here = fr.at[y, xl, z, xh]
        send(here, here, (lat, wrap(lon + i, 16)), kf + i - 1)
    mark("s28_pump")
    mark("s29_fwait")
    for i in range(1, 16):
        o = wrap(lon - i, 16)
        arrived(fr.at[y, xl, o // 2, lax.rem(o, 2)], kf + i - 1)
    kg = take(7)
    for i in range(1, 8):
        g = wrap(lat // 2 + i, 8)
        send(fr.at[y, xl], fr.at[y, xl], (g * 2 + core, lon), kg + i - 1)
    mark("s30_pump")
    pump("a", 7)
    pump("c", 7)
    pump("b", 13)
    for c in own_cov:
        c.wait()
    for g in range(8):
        arrived(cmat.at[g, pl.ds(pl.multiple_of((1 - core) * 64, 64), 64), :], k_cov + g)

    mark("s31_product")
    pacc[...] = jnp.zeros((2, 64, 512), F32)

    def product(g, carry):
        gy, gx = g // 2, lax.rem(g, 2)
        c = cmat[g]
        r0 = jnp.concatenate(
            [b0[gy, gx][:, :, 0:64].reshape(1024, 128), b1[gy, gx].reshape(1024, 128)], axis=1
        )
        left = dot(c, r0)
        pacc[0, :, 0:256] += left[0:64]
        pacc[1, :, 0:256] += left[64:128]
        tails = b0[gy, gx][:, :, 64:80].reshape(256, 128)
        pieces = []
        for q in range(4):
            sel = (
                lax.broadcasted_iota(jnp.int32, (128, 128), 0)
                == lax.broadcasted_iota(jnp.int32, (128, 128), 1) + 32 * q
            ).astype(F32).astype(BF16)
            pieces.append(dot(tails, sel).astype(BF16).reshape(16, 16, 128))
        last = jnp.concatenate(pieces, axis=1).reshape(1024, 128)
        right = dot(c, jnp.concatenate([b2[gy, gx].reshape(1024, 128), last], axis=1))
        pacc[0, :, 256:512] += right[0:64]
        pacc[1, :, 256:512] += right[64:128]
        return carry

    lax.fori_loop(0, 8, product, 0)
    kp = take()
    send(pacc.at[1 - core], precv, other, kp)

    mark("s32_f2wait")
    for i in range(1, 8):
        g = wrap(lat // 2 - i, 8)
        arrived(fr.at[g // 2, lax.rem(g, 2)], kg + i - 1)

    mark("s33_freshprod")

    def fresh_product(g, acc):
        f = fr[g // 2, lax.rem(g, 2)].reshape(16, 8, 128)
        lanes = lax.broadcasted_iota(jnp.int32, (16, 8, 128), 2) // 8
        w = jnp.concatenate([jnp.where(lanes == v, f, 0.0) for v in range(8)], axis=1)
        return acc + dot(cmat[g], w.astype(BF16).reshape(1024, 128))

    added = lax.fori_loop(0, 8, fresh_product, jnp.zeros((128, 128), F32))
    for shift in (64, 32, 16, 8):
        added = added + pltpu.roll(added, shift, 1)
    aacc[0] = added[0:64]
    aacc[1] = added[64:128]
    mark("s34_exch")
    ka = take()
    send(aacc.at[1 - core], arecv, other, ka)
    arrived(precv, kp)
    arrived(arecv, ka)
    mark("s35_final")
    mine = aacc[core] + arecv[...]
    base = pacc[core] + precv[...]
    for n in range(4):
        week_of = (lax.broadcasted_iota(jnp.int32, (64, 128), 1) + 128 * n) // 8
        pre[:, 128 * n:128 * n + 128] = base[:, 128 * n:128 * n + 128] + jnp.where(
            week_of == jnp.broadcast_to(week[...], (64, 128)), mine, 0.0
        )
    out_pre = load(pre, pre_h, 19)
    for c in sends:
        c.wait_send()
    out_field.wait()
    out_pre.wait()
    mark("")


COPIES = 240
UNROLL = 4
PROFILE = False


def shards(adjoint, transport, cell_weight, region_local, tile_regions, polar_rows, week_index, grad_in, covariance):
    hbm = pl.BlockSpec(memory_space=pl.ANY)
    aout, pre = pl.pallas_call(
        kernel,
        out_shape=(
            jax.ShapeDtypeStruct((8, 8, 32, 128), F32),
            jax.ShapeDtypeStruct((64, 512), F32),
        ),
        in_specs=[hbm] * 9,
        out_specs=(hbm, hbm),
        scratch_shapes=[
            pltpu.VMEM((8, 8, 32, 128), F32),
            pltpu.VMEM((6, 8, 32, 128), F32),
            pltpu.VMEM((32, 128), F32),
            pltpu.VMEM((32, 128), jnp.int32),
            pltpu.VMEM((256, 128), jnp.int32),
            pltpu.VMEM((1, 128), jnp.int32),
            pltpu.VMEM((1, 128), jnp.int32),
            pltpu.VMEM((64, 416), BF16),
            pltpu.VMEM((8, 8, 32, 128), F32),
            pltpu.VMEM((8, 32, 128), F32),
            pltpu.VMEM((4, 2, 8, 2, 80, 128), BF16),
            pltpu.VMEM((4, 2, 8, 2, 64, 128), BF16),
            pltpu.VMEM((4, 2, 8, 2, 64, 128), BF16),
            pltpu.VMEM((8, 128, 1024), BF16),
            pltpu.VMEM((4, 2, 8, 2, 8, 128), F32),
            pltpu.VMEM((4, 32, 128), F32),
            pltpu.VMEM((2, 64, 128), F32),
            pltpu.VMEM((2, 64, 128), F32),
            pltpu.VMEM((4, 32, 128), F32),
            pltpu.VMEM((4, 32, 128), F32),
            pltpu.VMEM((2, 64, 128), F32),
            pltpu.VMEM((2, 64, 128), F32),
            pltpu.VMEM((16, 16, 128), F32),
            pltpu.VMEM((16, 8, 128), F32),
            pltpu.VMEM((16, 1, 128), F32),
            pltpu.VMEM((16, 1, 128), F32),
            pltpu.VMEM((16, 1, 128), F32),
            pltpu.VMEM((16, 1, 128), F32),
            pltpu.VMEM((2, 64, 512), F32),
            pltpu.VMEM((64, 512), F32),
            pltpu.VMEM((2, 64, 128), F32),
            pltpu.VMEM((64, 128), F32),
            pltpu.VMEM((8, 8, 32, 128), F32),
            pltpu.VMEM((64, 512), F32),
            pltpu.SemaphoreType.DMA((COPIES,)),
            pltpu.SemaphoreType.DMA((COPIES,)),
            pltpu.SemaphoreType.DMA((8,)),
            pltpu.SemaphoreType.DMA((20,)),
        ],
        compiler_params=pltpu.CompilerParams(
            collective_id=0, has_side_effects=True, vmem_limit_bytes=67043328
        ),
        name="window",
    )(
        adjoint, transport, cell_weight, region_local, tile_regions,
        jnp.pad(polar_rows, (0, 96)).reshape(1, 128),
        jnp.broadcast_to(week_index.reshape(1, 1), (1, 128)), grad_in, covariance,
    )
    return aout, pre[:, :416]


def solution(mesh):
    both = ("lat", "lon")
    return jax.shard_map(
        shards,
        mesh=mesh,
        in_specs=(
            P(None, None, "lat", "lon"), P(None, None, "lat", "lon"), P("lat", "lon"), P("lat", "lon"),
            P(), P("lat"), P(), P(both, None), P(both, None),
        ),
        out_specs=(P(None, None, "lat", "lon"), P(both, None)),
        check_vma=False,
    )
```

```python
import functools

import jax
import jax.numpy as jnp
from jax import lax
from jax.experimental import pallas as pl
from jax.experimental.pallas import tpu as pltpu
from jax.sharding import PartitionSpec as P

MESH = pl.DeviceIdType.MESH
F32 = jnp.float32
BF16 = jnp.bfloat16
ALL = slice(None)


def dot(a, b):
    return lax.dot_general(a, b, (((1,), (0,)), ((), ())), preferred_element_type=F32)


def dot_nt(a, b):
    return lax.dot_general(a, b, (((1,), (1,)), ((), ())), preferred_element_type=F32)


def kernel(
    adj_h, tr_h, weight_h, rl_h, tiles_h, polar_h, week_h, grad, cov,
    aout_h, pre_h,
    adj, tr, weight, rl, tiles, polar, week, gtail,
    first, surf, b0, b1, b2, cmat, fr, col_s, row_n, row_s, col_e, col_w, halo_n, halo_s,
    zbuf, ybar, mbuf, xbuf, ybuf, obuf, pacc, precv, aacc, arecv,
    aout, pre, ssem, rsem, lsem, insem,
):
    lat = lax.axis_index("lat")
    lon = lax.axis_index("lon")
    core = lax.rem(lat, 2)
    xl = lax.rem(lat // 2, 2)
    y = lat // 4
    z = lon // 2
    xh = lax.rem(lon, 2)
    x = xh * 2 + xl
    me = {"x": x, "y": y, "z": z}
    size = {"x": 4, "y": 4, "z": 8}
    counter = [0]
    sends = []

    def wrap(v, n):
        return lax.rem(v + 2 * n, n)

    def device(c, at_core):
        return ((c["y"] * 2 + lax.rem(c["x"], 2)) * 2 + at_core, c["z"] * 2 + c["x"] // 2)

    def remote(src, dst, to, k):
        return pltpu.make_async_remote_copy(
            src_ref=src, dst_ref=dst, send_sem=ssem.at[k], recv_sem=rsem.at[k],
            device_id=to, device_id_type=MESH,
        )

    def send(src, dst, to, k):
        remote(src, dst, to, k).start()

    def take(*sizes):
        k = counter[0]
        counter[0] += len(sizes)
        for i, view in enumerate(sizes):
            sends.append((view, k + i))
        return k

    def arrived(view, k):
        remote(view, view, (lat, lon), k).wait_recv()

    other = (lat + 1 - 2 * core, lon)

    cur = [None]

    def mark(n):
        if PROFILE:
            if cur[0] is not None:
                cur[0].__exit__(None, None, None)
            cur[0] = jax.named_scope(n) if n else None
            if n:
                cur[0].__enter__()

    mark("s00_entry")
    barrier = pltpu.get_barrier_semaphore()
    for k in range(1, 16):
        pl.semaphore_signal(barrier, inc=1, device_id=(lat, wrap(lon + k, 16)), device_id_type=MESH)
        pl.semaphore_signal(barrier, inc=1, device_id=(wrap(lat + k, 16), lon), device_id_type=MESH)
    pl.semaphore_signal(
        barrier, inc=1, device_id=(lat + 2 - 4 * xl, lon + 1 - 2 * xh), device_id_type=MESH
    )

    def load(src, dst, k):
        c = pltpu.make_async_copy(src, dst, insem.at[k])
        c.start()
        return c

    in_adj = [load(adj_h.at[:, l], adj.at[l], l) for l in range(8)]
    in_grad = [
        load(grad.at[:, 0:128], b0.at[y, xl, z, xh, 0:64], 8),
        load(grad.at[:, 128:256], b1.at[y, xl, z, xh], 9),
        load(grad.at[:, 256:384], b2.at[y, xl, z, xh], 10),
        load(grad, gtail, 11),
    ]
    in_tr = load(tr_h, tr, 12)
    number = lat * 16 + lon
    lanes_at = pl.multiple_of(number // 128 * 128, 128)
    in_late = [
        load(weight_h, weight, 13), load(rl_h, rl, 14), load(polar_h, polar, 15),
        load(tiles_h.at[:, pl.ds(lanes_at, 128)], tiles, 16), load(week_h, week, 17),
    ]
    for g in range(8):
        c = pltpu.make_async_copy(
            cov.at[:, pl.ds(pl.multiple_of((g * 2 + core) * 1024, 1024), 1024)],
            cmat.at[g, pl.ds(pl.multiple_of(core * 64, 64), 64), :],
            lsem.at[0],
        )
        c.start()

    lane = lax.broadcasted_iota(jnp.int32, (32, 128), 1)
    row = lax.broadcasted_iota(jnp.int32, (32, 128), 0)

    def edges(step, j, v, acc):
        row_n[step, pl.ds(j, 1), :] = v[31:32, :]
        row_s[step, pl.ds(j, 1), :] = v[0:1, :]
        return jnp.where(lane // 2 == j, pltpu.roll(v, lax.rem(2 * j + 1, 128), 1), acc)

    def pack(j, acc):
        return edges(0, j, adj[j // 8, lax.rem(j, 8)], acc)

    none = jnp.zeros((32, 128), F32)
    in_adj[0].wait()
    in_adj[1].wait()
    col_s[0] = lax.fori_loop(0, 16, pack, none, unroll=4)
    mark("s01_barrier")
    pl.semaphore_wait(barrier, 31)
    mark("s02_send1")

    east, west = wrap(lon + 1, 16), wrap(lon - 1, 16)
    north, south = wrap(lat + 1, 16), wrap(lat - 1, 16)

    def halo_send(s, i, lo, hi):
        rows = pl.ds(lo, hi - lo)
        cols = col_s.at[2 * s + i]
        k = take(cols, cols, row_n.at[s, rows], row_n.at[s, rows])
        send(row_n.at[s, rows], halo_s.at[s, rows], (north, lon), k + 2)
        send(row_s.at[s, rows], halo_n.at[s, rows], (south, lon), k + 3)
        send(col_s.at[2 * s + i], col_w.at[2 * s + i], (lat, east), k)
        send(col_s.at[2 * s + i], col_e.at[2 * s + i], (lat, west), k + 1)
        return k

    def halo_wait(s, i, lo, hi, k):
        rows = pl.ds(lo, hi - lo)
        arrived(col_w.at[2 * s + i], k)
        arrived(col_e.at[2 * s + i], k + 1)
        arrived(halo_s.at[s, rows], k + 2)
        arrived(halo_n.at[s, rows], k + 3)
        return jnp.where(lax.rem(lane, 2) == 1, col_e[2 * s + i], pltpu.roll(col_w[2 * s + i], 2, 1))

    parts = {
        "a": (b0, "zyx", 48),
        "b": (b1, "yxz", 32),
        "c": (b2, "xzy", 32),
    }

    def slot(buf, at, rows):
        yi = at["y"] if at["y"] is not None else ALL
        zi = at["z"] if at["z"] is not None else ALL
        if at["x"] is None:
            return buf.at[yi, :, zi, :, rows]
        return buf.at[yi, lax.rem(at["x"], 2), zi, at["x"] // 2, rows]

    def whole(buf):
        return pl.ds(0, buf.shape[4])

    ids = {}

    singles = {"a": b0.at[0, 0, 0:7, 0], "b": b1.at[0:3, 0, 0, 0], "c": b2.at[0, 0, 0:3, 0]}
    views = {
        "a": {1: b0.at[0, 0, :, 0], 2: b0.at[0, 0], 4: b0.at[0]},
        "b": {1: b1.at[:, 0, 0, 0], 2: b1.at[:, 0, 0], 4: b1.at[:, :, 0]},
        "c": {1: b2.at[0, :, 0], 2: b2.at[0, 0, 0:4], 4: b2.at[0, 0]},
    }

    def direct_start(p):
        buf, order, _ = parts[p]
        d = order[0]
        n = size[d]
        k = take(singles[p])
        ids[p, 1] = k
        for i in range(1, n):
            to = dict(me)
            to[d] = wrap(me[d] + i, n)
            here = slot(buf, me, whole(buf))
            send(here, here, device(to, core), k)

    def direct_wait(p):
        arrived(singles[p], ids[p, 1])

    groups = {4: ((0,), (1, 3), (2,)), 8: ((0,), (1, 7), (2, 6), (3, 5), (4,))}

    def offsets(p, stage, g):
        return groups[size[parts[p][1][1]]][g] if stage == 3 else (0,)

    def unit(p, stage, s, g):
        n = size[parts[p][1][stage - 1]]
        return views[p][len(offsets(p, stage, g)) * (1 if s == n // 2 else 2)]

    def ring(p, stage, s, off):
        buf, order, half = parts[p]
        d = order[stage - 1]
        n = size[d]
        at = {c: (None if c in order[:stage - 1] else me[c]) for c in "xyz"}
        if stage == 3:
            at[order[1]] = wrap(me[order[1]] + off, size[order[1]])
        last = s == n // 2
        rows_r = pl.ds(0, half) if last else whole(buf)
        rows_l = pl.ds(half, buf.shape[4] - half) if last else whole(buf)
        return buf, d, n, at, rows_r, rows_l

    def ring_start(p, stage, s, g):
        k = take(unit(p, stage, s, g))
        ids[p, stage, s, g] = k
        for off in offsets(p, stage, g):
            buf, d, n, at, rows_r, rows_l = ring(p, stage, s, off)
            right, left = dict(me), dict(me)
            right[d] = wrap(me[d] + 1, n)
            left[d] = wrap(me[d] - 1, n)
            fwd, back = dict(at), dict(at)
            fwd[d] = wrap(me[d] - (s - 1), n)
            back[d] = wrap(me[d] + (s - 1), n)
            src = slot(buf, fwd, rows_r)
            send(src, src, device(right, core), k)
            src = slot(buf, back, rows_l)
            send(src, src, device(left, core), k)

    def ring_wait(p, stage, s, g):
        arrived(unit(p, stage, s, g), ids[p, stage, s, g])

    short = (
        ((), ((2, 1, 0), (3, 1, 0))),
        (((2, 1, 0),), ((2, 2, 0), (3, 1, 1))),
        (((3, 1, 0),), ((3, 2, 0),)),
        (((2, 2, 0),), ((3, 1, 2),)),
        (((3, 1, 1),), ((3, 2, 1),)),
        (((3, 1, 2),), ((3, 2, 2),)),
        (((3, 2, 0), (3, 2, 1), (3, 2, 2)), ()),
    )
    long = short[:3] + (
        short[3],
        short[4],
        (((3, 2, 0),), ((3, 3, 0),)),
        (((3, 1, 2),), ((3, 2, 2),)),
        (((3, 2, 1),), ((3, 3, 1),)),
        (((3, 3, 0),), ((3, 4, 0),)),
        (((3, 2, 2),), ((3, 3, 2),)),
        (((3, 3, 1),), ((3, 4, 1),)),
        (((3, 3, 2),), ((3, 4, 2),)),
        (((3, 4, 0), (3, 4, 1), (3, 4, 2)), ()),
    )
    other_way = (
        ((), ((2, 1, 0), (3, 1, 0))),
        (((2, 1, 0),), ((2, 2, 0), (3, 1, 1))),
        (((3, 1, 0),), ((3, 2, 0),)),
        (((2, 2, 0),), ((2, 3, 0), (3, 1, 2))),
        (((3, 1, 1),), ((3, 2, 1),)),
        (((2, 3, 0),), ((2, 4, 0), (3, 1, 3))),
        (((3, 1, 2),), ((3, 2, 2),)),
        (((2, 4, 0),), ((3, 1, 4),)),
        (((3, 1, 3),), ((3, 2, 3),)),
        (((3, 1, 4),), ((3, 2, 4),)),
        (((3, 2, 0), (3, 2, 1), (3, 2, 2), (3, 2, 3), (3, 2, 4)), ()),
    )
    plan = {"a": short, "b": long, "c": other_way}

    def pump(p, *events):
        for i in events:
            waits, starts = plan[p][i - 1]
            if i == 1:
                direct_wait(p)
            for w in waits:
                ring_wait(p, *w)
            for w in starts:
                ring_start(p, *w)

    k1a = halo_send(0, 0, 0, 16)
    for c in in_adj[2:]:
        c.wait()
    col_s[1] = lax.fori_loop(16, 64, pack, none, unroll=4)

    for c in in_grad:
        c.wait()
    tail = jnp.zeros((16, 128), F32)
    for q in range(4):
        sel = (
            lax.broadcasted_iota(jnp.int32, (32, 128), 1)
            == lax.broadcasted_iota(jnp.int32, (32, 128), 0) + 32 * q
        ).astype(F32).astype(BF16)
        tail = tail + dot(gtail[16 * q:16 * q + 16, 384:416], sel)
    b0[y, xl, z, xh, 64:80, :] = tail.astype(BF16)

    k1b = halo_send(0, 1, 16, 64)
    for p in "bac":
        direct_start(p)
    k_cov = take(cmat.at[:, 0:64])
    for g in range(8):
        send(
            cov.at[:, pl.ds(pl.multiple_of((g * 2 + 1 - core) * 1024, 1024), 1024)],
            cmat.at[g, pl.ds(pl.multiple_of(core * 64, 64), 64), :],
            other, k_cov,
        )

    has_north = (lat < 15).astype(F32)
    has_south = (lat > 0).astype(F32)

    def stencil(src, step, j, sides):
        l, t = j // 8, lax.rem(j, 8)
        c = src[l, t]
        h = pltpu.roll(sides, 126 - 2 * j, 1)
        e = jnp.where(lane == 127, h, pltpu.roll(c, 127, 1))
        v = jnp.where(lane == 0, h, pltpu.roll(c, 1, 1))
        n = jnp.where(row == 31, has_north * halo_n[step, pl.ds(j, 1), :], pltpu.roll(c, 31, 0))
        s = jnp.where(row == 0, has_south * halo_s[step, pl.ds(j, 1), :], pltpu.roll(c, 1, 0))
        u = src[jnp.minimum(l + 1, 7), t]
        d = src[jnp.maximum(l - 1, 0), t]
        return (
            c + tr[0, l] * (e - c) + tr[1, l] * (v - c) + tr[2, l] * (n - c)
            + tr[3, l] * (s - c) + tr[4, l] * (u - c) + tr[5, l] * (d - c)
        )

    mark("s03_halo1a")
    in_tr.wait()
    sides1a = halo_wait(0, 0, 0, 16, k1a)
    mark("s04_step1a")

    def step_one(sides):
        def body(j, acc):
            v = stencil(adj, 0, j, sides)
            first[j // 8, lax.rem(j, 8)] = v
            return edges(1, j, v, acc)
        return body

    col_s[2] = lax.fori_loop(0, 8, step_one(sides1a), none, unroll=UNROLL)
    k2a = halo_send(1, 0, 0, 8)
    mark("s05_step1a2")
    rest1 = lax.fori_loop(8, 16, step_one(sides1a), none, unroll=UNROLL)
    mark("s06_pump")
    pump("b", 1)
    pump("c", 1)
    mark("s07_halo1b")
    sides1b = halo_wait(0, 1, 16, 64, k1b)
    mark("s08_step1b")
    col_s[3] = lax.fori_loop(16, 64, step_one(sides1b), rest1, unroll=UNROLL)
    k2b = halo_send(1, 1, 8, 64)
    mark("s09_pump")
    pump("a", 1)
    pump("b", 2)
    pump("c", 2)
    mark("s10_halo2a")
    sides2a = halo_wait(1, 0, 0, 8, k2a)
    mark("s11_step2a")

    def step_two(sides):
        def body(j, acc):
            v = stencil(first, 1, j, sides)
            aout[lax.rem(j, 8), j // 8] = v
            return jnp.where(lane == j, jnp.sum(v, axis=1, keepdims=True), acc)
        return body

    sums = lax.fori_loop(0, 8, step_two(sides2a), none, unroll=UNROLL)
    lane8 = lax.broadcasted_iota(jnp.int32, (8, 128), 1)
    row8 = lax.broadcasted_iota(jnp.int32, (8, 128), 0)
    tight = sums[0:8]
    for i in range(1, 4):
        tight = jnp.where(lane8 // 8 == i, pltpu.roll(sums[8 * i:8 * i + 8], 8 * i, 1), tight)
    ybar[lon] = tight
    kz = take(ybar.at[0:15])
    for i in range(1, 16):
        send(ybar.at[lon], ybar.at[lon], (lat, wrap(lon + i, 16)), kz)
    mark("s12_pump")
    pump("b", 3)
    pump("c", 3)
    mark("s15_pump")
    pump("b", 4)
    pump("c", 4)
    for c in in_late:
        c.wait()
    flags = 0.5 * jnp.sum(
        jnp.where(
            lax.broadcasted_iota(jnp.int32, (32, 32), 0) == lax.broadcasted_iota(jnp.int32, (32, 32), 1),
            jnp.broadcast_to(polar[...], (32, 32)), 0,
        ).astype(F32), axis=1, keepdims=True
    )
    lane256 = lax.broadcasted_iota(jnp.int32, (256, 128), 1)
    row256 = lax.broadcasted_iota(jnp.int32, (256, 128), 0)
    mine_at = jnp.sum(
        jnp.where(lane256 == number - lanes_at, tiles[...] - 64 * number, 0).astype(F32), axis=1, keepdims=True
    )
    spread = jnp.where(lane256 // 8 == lax.rem(row256, 16), mine_at, 0.0).astype(BF16)
    pick = (
        lax.broadcasted_iota(jnp.int32, (16, 256), 1) // 16 == lax.broadcasted_iota(jnp.int32, (16, 256), 0)
    ).astype(F32).astype(BF16)
    reg = dot(pick, spread).astype(jnp.int32)
    mark("s16_zwait")
    arrived(ybar.at[0:15], kz)
    mark("s17_surf")
    total = ybar[0]
    for i in range(1, 16):
        total = total + ybar[i]
    total = total * (1.0 / 2048.0)
    mean0 = jnp.concatenate([total] + [pltpu.roll(total, 128 - 8 * i, 1) for i in range(1, 4)], axis=0)

    def filtered(j, mean):
        v = aout[lax.rem(j, 8), j // 8]
        v = v + flags * (jnp.sum(jnp.where(lane == j, mean, 0.0), axis=1, keepdims=True) - v)
        aout[lax.rem(j, 8), j // 8] = v
        return v

    for t in range(8):
        surf[t] = filtered(t, mean0) * weight[...]

    mark("s18_pump")
    pump("a", 2)
    pump("b", 5)
    pump("c", 5)
    mark("s19_regions")

    sub8 = lax.broadcasted_iota(jnp.int32, (16, 128), 0)

    def regions(r, acc):
        lhs, rhs = [], [[], [], []]
        for h in range(2):
            i = 2 * r + h
            local = rl[pl.ds(i, 1), :]
            low = jnp.broadcast_to(local & 15, (16, 128))
            high = jnp.broadcast_to(local >> 4, (8, 128))
            lhs.append((low == sub8).astype(F32).astype(BF16))
            s = jnp.concatenate([surf[t, pl.ds(i, 1), :] for t in range(8)], axis=0)
            for n in range(3):
                piece = s.astype(BF16).astype(F32)
                s = s - piece
                rhs[n].append(
                    jnp.concatenate([jnp.where(high == a, piece, 0.0) for a in range(16)], axis=0).astype(BF16)
                )
        left = jnp.concatenate(lhs, axis=1)
        for n in range(3):
            acc = acc + dot_nt(left, jnp.concatenate(rhs[n], axis=1))
        return acc

    m = lax.fori_loop(0, 16, regions, jnp.zeros((16, 128), F32), unroll=2)
    for i in range(16):
        mbuf[i] = m[i:i + 1, :]
    xbuf[lon] = mbuf[lon]
    kx = take(xbuf.at[0:15])
    for i in range(1, 16):
        to = wrap(lon + i, 16)
        send(mbuf.at[to], xbuf.at[lon], (lat, to), kx)

    mark("s13_halo2b")
    sides2b = halo_wait(1, 1, 8, 64, k2b)
    mark("s14_step2b")
    sums = lax.fori_loop(8, 64, step_two(sides2b), none, unroll=UNROLL)
    lane16 = lax.broadcasted_iota(jnp.int32, (16, 128), 1)
    row16 = lax.broadcasted_iota(jnp.int32, (16, 128), 0)
    zbuf[lon] = jnp.where(lane16 < 64, sums[0:16], pltpu.roll(sums[16:32], 64, 1))
    kw = take(zbuf.at[0:15])
    for i in range(1, 16):
        send(zbuf.at[lon], zbuf.at[lon], (lat, wrap(lon + i, 16)), kw)
    mark("s20_pump")
    pump("b", 6)
    pump("c", 6)
    pump("a", 3)
    pump("b", 7)
    pump("c", 7)
    mark("s22_pump")
    mark("s23_xwait")
    arrived(xbuf.at[0:15], kx)
    mark("s24_turn")
    got = jnp.concatenate([xbuf[i] for i in range(16)], axis=0)
    turned = jnp.zeros((16, 128), F32)
    group = lane16 // 8
    for d in range(16):
        moved = got if d == 0 else pltpu.roll(pltpu.roll(got, 16 - d, 0), 8 * d, 1)
        turned = jnp.where(lax.rem(group - row16 + 16, 16) == d, moved, turned)
    for i in range(16):
        ybuf[i] = turned[i:i + 1, :]
    obuf[lat] = ybuf[lat]
    ky = take(obuf.at[0:15])
    for i in range(1, 16):
        to = wrap(lat + i, 16)
        send(ybuf.at[to], obuf.at[lat], (to, lon), ky)
    mark("s25_pump")
    pump("a", 4)
    pump("b", 8)
    pump("c", 8)
    pump("b", 9)
    mark("s21_rest")
    arrived(zbuf.at[0:15], kw)
    total = zbuf[0]
    for i in range(1, 16):
        total = total + zbuf[i]
    total = total * (1.0 / 2048.0)
    mean = jnp.concatenate([total, pltpu.roll(total, 64, 1)], axis=0)

    def rest(j, carry):
        filtered(j, mean)
        return carry

    lax.fori_loop(8, 64, rest, 0, unroll=UNROLL)
    out_field = load(aout, aout_h, 18)
    mark("s26_owait")
    pump("a", 5)
    pump("c", 9)
    pump("b", 10)
    arrived(obuf.at[0:15], ky)

    mark("s27_fresh")
    packed = jnp.zeros((8, 128), F32)
    for v in range(8):
        f = jnp.zeros((8, 128), F32)
        for a in range(16):
            f = f + jnp.where(reg[a:a + 1, :] == row8 + 8 * v, obuf[a], 0.0)
        for shift in (64, 32, 16, 8):
            f = f + pltpu.roll(f, shift, 1)
        packed = jnp.where(lane8 // 8 == v, f, packed)
    packed = packed.astype(BF16).astype(F32)
    fr[y, xl, z, xh] = packed[0:4] + pltpu.roll(packed[4:8], 64, 1)
    kf = take(fr.at[0:3, 0, 0:5, 0])
    for i in range(1, 16):
        here = fr.at[y, xl, z, xh]
        send(here, here, (lat, wrap(lon + i, 16)), kf)
    mark("s28_pump")
    pump("a", 6)
    pump("c", 10)
    pump("b", 11)
    pump("b", 12)
    mark("s29_fwait")
    arrived(fr.at[0:3, 0, 0:5, 0], kf)
    kg = take(fr.at[:, :, 0:7])
    for i in range(1, 8):
        g = wrap(lat // 2 + i, 8)
        send(fr.at[y, xl], fr.at[y, xl], (g * 2 + core, lon), kg)
    mark("s30_pump")
    pump("a", 7)
    pump("c", 11)
    pump("b", 13)
    pltpu.make_async_copy(cmat.at[:, 0:64], cmat.at[:, 0:64], lsem.at[0]).wait()
    arrived(cmat.at[:, 0:64], k_cov)

    mark("s31_product")
    pacc[...] = jnp.zeros((2, 64, 512), F32)

    def product(g, carry):
        gy, gx = g // 2, lax.rem(g, 2)
        c = cmat[g]
        r0 = jnp.concatenate(
            [b0[gy, gx][:, :, 0:64].reshape(1024, 128), b1[gy, gx].reshape(1024, 128)], axis=1
        )
        left = dot(c, r0)
        pacc[0, :, 0:256] += left[0:64]
        pacc[1, :, 0:256] += left[64:128]
        tails = b0[gy, gx][:, :, 64:80].reshape(256, 128)
        pieces = []
        for q in range(4):
            sel = (
                lax.broadcasted_iota(jnp.int32, (128, 128), 0)
                == lax.broadcasted_iota(jnp.int32, (128, 128), 1) + 32 * q
            ).astype(F32).astype(BF16)
            pieces.append(dot(tails, sel).astype(BF16).reshape(16, 16, 128))
        last = jnp.concatenate(pieces, axis=1).reshape(1024, 128)
        right = dot(c, jnp.concatenate([b2[gy, gx].reshape(1024, 128), last], axis=1))
        pacc[0, :, 256:512] += right[0:64]
        pacc[1, :, 256:512] += right[64:128]
        return carry

    lax.fori_loop(0, 8, product, 0)
    kp = take(precv)
    send(pacc.at[1 - core], precv, other, kp)

    mark("s32_f2wait")
    arrived(fr.at[:, :, 0:7], kg)

    mark("s33_freshprod")

    def fresh_product(g, acc):
        f = fr[g // 2, lax.rem(g, 2)].reshape(16, 4, 128)
        f = jnp.concatenate([f, f], axis=1)
        lanes = (
            lax.broadcasted_iota(jnp.int32, (16, 8, 128), 2) // 8
            - lax.broadcasted_iota(jnp.int32, (16, 8, 128), 1) // 4 * 8
        )
        w = jnp.concatenate([jnp.where(lanes == v, f, 0.0) for v in range(8)], axis=1)
        return acc + dot(cmat[g], w.astype(BF16).reshape(1024, 128))

    added = lax.fori_loop(0, 8, fresh_product, jnp.zeros((128, 128), F32), unroll=2)
    for shift in (64, 32, 16, 8):
        added = added + pltpu.roll(added, shift, 1)
    aacc[0] = added[0:64]
    aacc[1] = added[64:128]
    mark("s34_exch")
    ka = take(arecv)
    send(aacc.at[1 - core], arecv, other, ka)
    arrived(precv, kp)
    arrived(arecv, ka)
    mark("s35_final")
    mine = aacc[core] + arecv[...]
    base = pacc[core] + precv[...]
    for n in range(4):
        week_of = (lax.broadcasted_iota(jnp.int32, (64, 128), 1) + 128 * n) // 8
        pre[:, 128 * n:128 * n + 128] = base[:, 128 * n:128 * n + 128] + jnp.where(
            week_of == jnp.broadcast_to(week[...], (64, 128)), mine, 0.0
        )
    out_pre = load(pre, pre_h, 19)
    for view, k in sends:
        remote(view, view, (lat, lon), k).wait_send()
    out_field.wait()
    out_pre.wait()
    mark("")


COPIES = 64
UNROLL = 4
PROFILE = False


def shards(adjoint, transport, cell_weight, region_local, tile_regions, polar_rows, week_index, grad_in, covariance):
    hbm = pl.BlockSpec(memory_space=pl.ANY)
    aout, pre = pl.pallas_call(
        kernel,
        out_shape=(
            jax.ShapeDtypeStruct((8, 8, 32, 128), F32),
            jax.ShapeDtypeStruct((64, 512), F32),
        ),
        in_specs=[hbm] * 9,
        out_specs=(hbm, hbm),
        scratch_shapes=[
            pltpu.VMEM((8, 8, 32, 128), F32),
            pltpu.VMEM((6, 8, 32, 128), F32),
            pltpu.VMEM((32, 128), F32),
            pltpu.VMEM((32, 128), jnp.int32),
            pltpu.VMEM((256, 128), jnp.int32),
            pltpu.VMEM((1, 32), jnp.int32),
            pltpu.VMEM((1, 1), jnp.int32),
            pltpu.VMEM((64, 416), BF16),
            pltpu.VMEM((8, 8, 32, 128), F32),
            pltpu.VMEM((8, 32, 128), F32),
            pltpu.VMEM((4, 2, 8, 2, 80, 128), BF16),
            pltpu.VMEM((4, 2, 8, 2, 64, 128), BF16),
            pltpu.VMEM((4, 2, 8, 2, 64, 128), BF16),
            pltpu.VMEM((8, 128, 1024), BF16),
            pltpu.VMEM((4, 2, 8, 2, 4, 128), F32),
            pltpu.VMEM((4, 32, 128), F32),
            pltpu.VMEM((2, 64, 128), F32),
            pltpu.VMEM((2, 64, 128), F32),
            pltpu.VMEM((4, 32, 128), F32),
            pltpu.VMEM((4, 32, 128), F32),
            pltpu.VMEM((2, 64, 128), F32),
            pltpu.VMEM((2, 64, 128), F32),
            pltpu.VMEM((16, 16, 128), F32),
            pltpu.VMEM((16, 8, 128), F32),
            pltpu.VMEM((16, 1, 128), F32),
            pltpu.VMEM((16, 1, 128), F32),
            pltpu.VMEM((16, 1, 128), F32),
            pltpu.VMEM((16, 1, 128), F32),
            pltpu.VMEM((2, 64, 512), F32),
            pltpu.VMEM((64, 512), F32),
            pltpu.VMEM((2, 64, 128), F32),
            pltpu.VMEM((64, 128), F32),
            pltpu.VMEM((8, 8, 32, 128), F32),
            pltpu.VMEM((64, 512), F32),
            pltpu.SemaphoreType.DMA((COPIES,)),
            pltpu.SemaphoreType.DMA((COPIES,)),
            pltpu.SemaphoreType.DMA((1,)),
            pltpu.SemaphoreType.DMA((20,)),
        ],
        compiler_params=pltpu.CompilerParams(
            collective_id=0, has_side_effects=True, vmem_limit_bytes=67043328
        ),
        name="window",
    )(
        adjoint, transport, cell_weight, region_local, tile_regions,
        polar_rows.reshape(1, 32), week_index.reshape(1, 1), grad_in, covariance,
    )
    return aout, pre[:, :416]


def solution(mesh):
    both = ("lat", "lon")
    return jax.shard_map(
        shards,
        mesh=mesh,
        in_specs=(
            P(None, None, "lat", "lon"), P(None, None, "lat", "lon"), P("lat", "lon"), P("lat", "lon"),
            P(), P("lat"), P(), P(both, None), P(both, None),
        ),
        out_specs=(P(None, None, "lat", "lon"), P(both, None)),
        check_vma=False,
    )
```

```python
import functools

import jax
import jax.numpy as jnp
from jax import lax
from jax.experimental import pallas as pl
from jax.experimental.pallas import tpu as pltpu
from jax.sharding import PartitionSpec as P

MESH = pl.DeviceIdType.MESH
F32 = jnp.float32
BF16 = jnp.bfloat16
ALL = slice(None)


def dot(a, b):
    return lax.dot_general(a, b, (((1,), (0,)), ((), ())), preferred_element_type=F32)


def dot_nt(a, b):
    return lax.dot_general(a, b, (((1,), (1,)), ((), ())), preferred_element_type=F32)


def kernel(
    adj_h, tr_h, weight_h, rl_h, tiles_h, polar_h, week_h, grad, cov,
    aout_h, pre_h,
    adj, tr, weight, rl, tiles, polar, week, gtail,
    first, surf, b0, b1, b2, cmat, fr, col_s, row_n, row_s, col_e, col_w, halo_n, halo_s,
    zbuf, ybar, mbuf, xbuf, ybuf, obuf, pacc, precv, aacc, arecv,
    aout, pre, ssem, rsem, lsem, insem,
):
    lat = lax.axis_index("lat")
    lon = lax.axis_index("lon")
    core = lax.rem(lat, 2)
    xl = lax.rem(lat // 2, 2)
    y = lat // 4
    z = lon // 2
    xh = lax.rem(lon, 2)
    x = xh * 2 + xl
    me = {"x": x, "y": y, "z": z}
    size = {"x": 4, "y": 4, "z": 8}
    counter = [0]
    sends = []

    def wrap(v, n):
        return lax.rem(v + 2 * n, n)

    def device(c, at_core):
        return ((c["y"] * 2 + lax.rem(c["x"], 2)) * 2 + at_core, c["z"] * 2 + c["x"] // 2)

    def remote(src, dst, to, k):
        return pltpu.make_async_remote_copy(
            src_ref=src, dst_ref=dst, send_sem=ssem.at[k], recv_sem=rsem.at[k],
            device_id=to, device_id_type=MESH,
        )

    def send(src, dst, to, k):
        remote(src, dst, to, k).start()

    def take(*sizes):
        k = counter[0]
        counter[0] += len(sizes)
        for i, view in enumerate(sizes):
            sends.append((view, k + i))
        return k

    def arrived(view, k):
        remote(view, view, (lat, lon), k).wait_recv()

    other = (lat + 1 - 2 * core, lon)

    cur = [None]

    def mark(n):
        if PROFILE:
            if cur[0] is not None:
                cur[0].__exit__(None, None, None)
            cur[0] = jax.named_scope(n) if n else None
            if n:
                cur[0].__enter__()

    mark("s00_entry")
    barrier = pltpu.get_barrier_semaphore()
    for k in range(1, 16):
        pl.semaphore_signal(barrier, inc=1, device_id=(lat, wrap(lon + k, 16)), device_id_type=MESH)
        pl.semaphore_signal(barrier, inc=1, device_id=(wrap(lat + k, 16), lon), device_id_type=MESH)
    pl.semaphore_signal(
        barrier, inc=1, device_id=(lat + 2 - 4 * xl, lon + 1 - 2 * xh), device_id_type=MESH
    )

    def load(src, dst, k):
        c = pltpu.make_async_copy(src, dst, insem.at[k])
        c.start()
        return c

    in_adj = [load(adj_h.at[:, l], adj.at[l], l) for l in range(8)]
    in_grad = [
        load(grad.at[:, 0:128], b0.at[y, xl, z, xh, 0:64], 8),
        load(grad.at[:, 128:256], b1.at[y, xl, z, xh], 9),
        load(grad.at[:, 256:384], b2.at[y, xl, z, xh], 10),
        load(grad, gtail, 11),
    ]
    in_tr = load(tr_h, tr, 12)
    number = lat * 16 + lon
    lanes_at = pl.multiple_of(number // 128 * 128, 128)
    in_late = [
        load(weight_h, weight, 13), load(rl_h, rl, 14), load(polar_h, polar, 15),
        load(tiles_h.at[:, pl.ds(lanes_at, 128)], tiles, 16), load(week_h, week, 17),
    ]
    for g in range(8):
        c = pltpu.make_async_copy(
            cov.at[:, pl.ds(pl.multiple_of((g * 2 + core) * 1024, 1024), 1024)],
            cmat.at[g, pl.ds(pl.multiple_of(core * 64, 64), 64), :],
            lsem.at[0],
        )
        c.start()

    lane = lax.broadcasted_iota(jnp.int32, (32, 128), 1)
    row = lax.broadcasted_iota(jnp.int32, (32, 128), 0)

    def edges(step, j, v, acc):
        row_n[step, pl.ds(j, 1), :] = v[31:32, :]
        row_s[step, pl.ds(j, 1), :] = v[0:1, :]
        return jnp.where(lane // 2 == j, pltpu.roll(v, lax.rem(2 * j + 1, 128), 1), acc)

    def pack(j, acc):
        return edges(0, j, adj[j // 8, lax.rem(j, 8)], acc)

    none = jnp.zeros((32, 128), F32)
    in_adj[0].wait()
    in_adj[1].wait()
    col_s[0] = lax.fori_loop(0, 16, pack, none, unroll=4)
    mark("s01_barrier")
    pl.semaphore_wait(barrier, 31)
    mark("s02_send1")

    east, west = wrap(lon + 1, 16), wrap(lon - 1, 16)
    north, south = wrap(lat + 1, 16), wrap(lat - 1, 16)

    def halo_send(s, i, lo, hi):
        rows = pl.ds(lo, hi - lo)
        cols = col_s.at[2 * s + i]
        k = take(cols, cols, row_n.at[s, rows], row_n.at[s, rows])
        send(row_n.at[s, rows], halo_s.at[s, rows], (north, lon), k + 2)
        send(row_s.at[s, rows], halo_n.at[s, rows], (south, lon), k + 3)
        send(col_s.at[2 * s + i], col_w.at[2 * s + i], (lat, east), k)
        send(col_s.at[2 * s + i], col_e.at[2 * s + i], (lat, west), k + 1)
        return k

    def halo_wait(s, i, lo, hi, k):
        rows = pl.ds(lo, hi - lo)
        arrived(col_w.at[2 * s + i], k)
        arrived(col_e.at[2 * s + i], k + 1)
        arrived(halo_s.at[s, rows], k + 2)
        arrived(halo_n.at[s, rows], k + 3)
        return jnp.where(lax.rem(lane, 2) == 1, col_e[2 * s + i], pltpu.roll(col_w[2 * s + i], 2, 1))

    parts = {
        "a": (b0, "zyx", 48),
        "b": (b1, "yxz", 32),
        "c": (b2, "xzy", 32),
    }

    def slot(buf, at, rows):
        yi = at["y"] if at["y"] is not None else ALL
        zi = at["z"] if at["z"] is not None else ALL
        if at["x"] is None:
            return buf.at[yi, :, zi, :, rows]
        return buf.at[yi, lax.rem(at["x"], 2), zi, at["x"] // 2, rows]

    def whole(buf):
        return pl.ds(0, buf.shape[4])

    ids = {}

    singles = {"a": b0.at[0, 0, 0:7, 0], "b": b1.at[0:3, 0, 0, 0], "c": b2.at[0, 0, 0:3, 0]}
    views = {
        "a": {1: b0.at[0, 0, :, 0], 2: b0.at[0, 0], 4: b0.at[0]},
        "b": {1: b1.at[:, 0, 0, 0], 2: b1.at[:, 0, 0], 4: b1.at[:, :, 0]},
        "c": {1: b2.at[0, :, 0], 2: b2.at[0, 0, 0:4], 4: b2.at[0, 0]},
    }

    def direct_start(p):
        buf, order, _ = parts[p]
        d = order[0]
        n = size[d]
        k = take(singles[p])
        ids[p, 1] = k
        for i in range(1, n):
            to = dict(me)
            to[d] = wrap(me[d] + i, n)
            here = slot(buf, me, whole(buf))
            send(here, here, device(to, core), k)

    def direct_wait(p):
        arrived(singles[p], ids[p, 1])

    groups = {4: ((0,), (1, 3), (2,)), 8: ((0,), (1, 7), (2, 6), (3, 5), (4,))}

    def offsets(p, stage, g):
        return groups[size[parts[p][1][1]]][g] if stage == 3 else (0,)

    def unit(p, stage, s, g):
        n = size[parts[p][1][stage - 1]]
        return views[p][len(offsets(p, stage, g)) * (1 if s == n // 2 else 2)]

    def ring(p, stage, s, off):
        buf, order, half = parts[p]
        d = order[stage - 1]
        n = size[d]
        at = {c: (None if c in order[:stage - 1] else me[c]) for c in "xyz"}
        if stage == 3:
            at[order[1]] = wrap(me[order[1]] + off, size[order[1]])
        last = s == n // 2
        rows_r = pl.ds(0, half) if last else whole(buf)
        rows_l = pl.ds(half, buf.shape[4] - half) if last else whole(buf)
        return buf, d, n, at, rows_r, rows_l

    def ring_start(p, stage, s, g):
        k = take(unit(p, stage, s, g))
        ids[p, stage, s, g] = k
        for off in offsets(p, stage, g):
            buf, d, n, at, rows_r, rows_l = ring(p, stage, s, off)
            right, left = dict(me), dict(me)
            right[d] = wrap(me[d] + 1, n)
            left[d] = wrap(me[d] - 1, n)
            fwd, back = dict(at), dict(at)
            fwd[d] = wrap(me[d] - (s - 1), n)
            back[d] = wrap(me[d] + (s - 1), n)
            src = slot(buf, fwd, rows_r)
            send(src, src, device(right, core), k)
            src = slot(buf, back, rows_l)
            send(src, src, device(left, core), k)

    def ring_wait(p, stage, s, g):
        arrived(unit(p, stage, s, g), ids[p, stage, s, g])

    short = (
        ((), ((2, 1, 0), (3, 1, 0))),
        (((2, 1, 0),), ((2, 2, 0), (3, 1, 1))),
        (((3, 1, 0),), ((3, 2, 0),)),
        (((2, 2, 0),), ((3, 1, 2),)),
        (((3, 1, 1),), ((3, 2, 1),)),
        (((3, 1, 2),), ((3, 2, 2),)),
        (((3, 2, 0), (3, 2, 1), (3, 2, 2)), ()),
    )
    long = (
        ((), ((2, 1, 0),)),
        (((2, 1, 0),), ((2, 2, 0),)),
        ((), ((3, 1, 0), (3, 1, 1))),
        (((2, 2, 0),), ((3, 1, 2),)),
        (((3, 1, 0),), ((3, 2, 0),)),
        (((3, 1, 1),), ((3, 2, 1),)),
        (((3, 2, 0),), ((3, 3, 0),)),
        (((3, 1, 2),), ((3, 2, 2),)),
        (((3, 2, 1),), ((3, 3, 1),)),
        (((3, 3, 0),), ((3, 4, 0),)),
        (((3, 2, 2),), ((3, 3, 2),)),
        (((3, 3, 1),), ((3, 4, 1),)),
        (((3, 3, 2),), ((3, 4, 2),)),
        (((3, 4, 0), (3, 4, 1), (3, 4, 2)), ()),
    )
    other_way = (
        ((), ((2, 1, 0), (3, 1, 0))),
        (((2, 1, 0),), ((2, 2, 0), (3, 1, 1))),
        (((3, 1, 0),), ((3, 2, 0),)),
        (((2, 2, 0),), ((2, 3, 0), (3, 1, 2))),
        (((3, 1, 1),), ((3, 2, 1),)),
        (((2, 3, 0),), ((2, 4, 0), (3, 1, 3))),
        (((3, 1, 2),), ((3, 2, 2),)),
        (((2, 4, 0),), ((3, 1, 4),)),
        (((3, 1, 3),), ((3, 2, 3),)),
        (((3, 1, 4),), ((3, 2, 4),)),
        (((3, 2, 0), (3, 2, 1), (3, 2, 2), (3, 2, 3), (3, 2, 4)), ()),
    )
    plan = {"a": short, "b": long, "c": other_way}

    def pump(p, *events):
        for i in events:
            waits, starts = plan[p][i - 1]
            if i == 1:
                direct_wait(p)
            for w in waits:
                ring_wait(p, *w)
            for w in starts:
                ring_start(p, *w)

    k1a = halo_send(0, 0, 0, 16)
    for c in in_adj[2:]:
        c.wait()
    col_s[1] = lax.fori_loop(16, 64, pack, none, unroll=4)

    for c in in_grad:
        c.wait()
    tail = jnp.zeros((16, 128), F32)
    for q in range(4):
        sel = (
            lax.broadcasted_iota(jnp.int32, (32, 128), 1)
            == lax.broadcasted_iota(jnp.int32, (32, 128), 0) + 32 * q
        ).astype(F32).astype(BF16)
        tail = tail + dot(gtail[16 * q:16 * q + 16, 384:416], sel)
    b0[y, xl, z, xh, 64:80, :] = tail.astype(BF16)

    k1b = halo_send(0, 1, 16, 64)
    for p in "bac":
        direct_start(p)
    k_cov = take(cmat.at[:, 0:64])
    for g in range(8):
        send(
            cov.at[:, pl.ds(pl.multiple_of((g * 2 + 1 - core) * 1024, 1024), 1024)],
            cmat.at[g, pl.ds(pl.multiple_of(core * 64, 64), 64), :],
            other, k_cov,
        )

    has_north = (lat < 15).astype(F32)
    has_south = (lat > 0).astype(F32)

    def stencil(src, step, j, sides):
        l, t = j // 8, lax.rem(j, 8)
        c = src[l, t]
        h = pltpu.roll(sides, 126 - 2 * j, 1)
        e = jnp.where(lane == 127, h, pltpu.roll(c, 127, 1))
        v = jnp.where(lane == 0, h, pltpu.roll(c, 1, 1))
        n = jnp.where(row == 31, has_north * halo_n[step, pl.ds(j, 1), :], pltpu.roll(c, 31, 0))
        s = jnp.where(row == 0, has_south * halo_s[step, pl.ds(j, 1), :], pltpu.roll(c, 1, 0))
        u = src[jnp.minimum(l + 1, 7), t]
        d = src[jnp.maximum(l - 1, 0), t]
        return (
            c + tr[0, l] * (e - c) + tr[1, l] * (v - c) + tr[2, l] * (n - c)
            + tr[3, l] * (s - c) + tr[4, l] * (u - c) + tr[5, l] * (d - c)
        )

    mark("s03_halo1a")
    in_tr.wait()
    sides1a = halo_wait(0, 0, 0, 16, k1a)
    mark("s04_step1a")

    def step_one(sides):
        def body(j, acc):
            v = stencil(adj, 0, j, sides)
            first[j // 8, lax.rem(j, 8)] = v
            return edges(1, j, v, acc)
        return body

    col_s[2] = lax.fori_loop(0, 8, step_one(sides1a), none, unroll=UNROLL)
    k2a = halo_send(1, 0, 0, 8)
    mark("s05_step1a2")
    rest1 = lax.fori_loop(8, 16, step_one(sides1a), none, unroll=UNROLL)
    mark("s06_pump")
    pump("b", 1)
    pump("c", 1)
    mark("s07_halo1b")
    sides1b = halo_wait(0, 1, 16, 64, k1b)
    mark("s08_step1b")
    col_s[3] = lax.fori_loop(16, 64, step_one(sides1b), rest1, unroll=UNROLL)
    k2b = halo_send(1, 1, 8, 64)
    mark("s09_pump")
    pump("b", 2)
    pump("c", 2)
    mark("s10_halo2a")
    sides2a = halo_wait(1, 0, 0, 8, k2a)
    mark("s11_step2a")

    def step_two(sides):
        def body(j, acc):
            v = stencil(first, 1, j, sides)
            aout[lax.rem(j, 8), j // 8] = v
            return jnp.where(lane == j, jnp.sum(v, axis=1, keepdims=True), acc)
        return body

    sums = lax.fori_loop(0, 8, step_two(sides2a), none, unroll=UNROLL)
    lane8 = lax.broadcasted_iota(jnp.int32, (8, 128), 1)
    row8 = lax.broadcasted_iota(jnp.int32, (8, 128), 0)
    tight = sums[0:8]
    for i in range(1, 4):
        tight = jnp.where(lane8 // 8 == i, pltpu.roll(sums[8 * i:8 * i + 8], 8 * i, 1), tight)
    ybar[lon] = tight
    kz = take(ybar.at[0:15])
    for i in range(1, 16):
        send(ybar.at[lon], ybar.at[lon], (lat, wrap(lon + i, 16)), kz)
    mark("s12_pump")
    pump("b", 3)
    pump("a", 1)
    pump("c", 3)
    pump("b", 4)
    mark("s15_pump")
    for c in in_late:
        c.wait()
    flags = 0.5 * jnp.sum(
        jnp.where(
            lax.broadcasted_iota(jnp.int32, (32, 32), 0) == lax.broadcasted_iota(jnp.int32, (32, 32), 1),
            jnp.broadcast_to(polar[...], (32, 32)), 0,
        ).astype(F32), axis=1, keepdims=True
    )
    lane256 = lax.broadcasted_iota(jnp.int32, (256, 128), 1)
    row256 = lax.broadcasted_iota(jnp.int32, (256, 128), 0)
    mine_at = jnp.sum(
        jnp.where(lane256 == number - lanes_at, tiles[...] - 64 * number, 0).astype(F32), axis=1, keepdims=True
    )
    spread = jnp.where(lane256 // 8 == lax.rem(row256, 16), mine_at, 0.0).astype(BF16)
    pick = (
        lax.broadcasted_iota(jnp.int32, (16, 256), 1) // 16 == lax.broadcasted_iota(jnp.int32, (16, 256), 0)
    ).astype(F32).astype(BF16)
    reg = dot(pick, spread).astype(jnp.int32)
    mark("s16_zwait")
    arrived(ybar.at[0:15], kz)
    mark("s17_surf")
    total = ybar[0]
    for i in range(1, 16):
        total = total + ybar[i]
    total = total * (1.0 / 2048.0)
    mean0 = jnp.concatenate([total] + [pltpu.roll(total, 128 - 8 * i, 1) for i in range(1, 4)], axis=0)

    def filtered(j, mean):
        v = aout[lax.rem(j, 8), j // 8]
        v = v + flags * (jnp.sum(jnp.where(lane == j, mean, 0.0), axis=1, keepdims=True) - v)
        aout[lax.rem(j, 8), j // 8] = v
        return v

    for t in range(8):
        surf[t] = filtered(t, mean0) * weight[...]

    mark("s18_pump")
    pump("c", 4)
    mark("s19_regions")

    sub8 = lax.broadcasted_iota(jnp.int32, (16, 128), 0)

    def regions(r, acc):
        lhs, rhs = [], [[], [], []]
        for h in range(2):
            i = 2 * r + h
            local = rl[pl.ds(i, 1), :]
            low = jnp.broadcast_to(local & 15, (16, 128))
            high = jnp.broadcast_to(local >> 4, (8, 128))
            lhs.append((low == sub8).astype(F32).astype(BF16))
            s = jnp.concatenate([surf[t, pl.ds(i, 1), :] for t in range(8)], axis=0)
            for n in range(3):
                piece = s.astype(BF16).astype(F32)
                s = s - piece
                rhs[n].append(
                    jnp.concatenate([jnp.where(high == a, piece, 0.0) for a in range(16)], axis=0).astype(BF16)
                )
        left = jnp.concatenate(lhs, axis=1)
        for n in range(3):
            acc = acc + dot_nt(left, jnp.concatenate(rhs[n], axis=1))
        return acc

    m = lax.fori_loop(0, 16, regions, jnp.zeros((16, 128), F32), unroll=4)
    for i in range(16):
        mbuf[i] = m[i:i + 1, :]
    xbuf[lon] = mbuf[lon]
    kx = take(xbuf.at[0:15])
    for i in range(1, 16):
        to = wrap(lon + i, 16)
        send(mbuf.at[to], xbuf.at[lon], (lat, to), kx)

    mark("s13_halo2b")
    pump("a", 2)
    pump("b", 5)
    pump("c", 5)
    pump("b", 6)
    sides2b = halo_wait(1, 1, 8, 64, k2b)
    mark("s14_step2b")
    sums = lax.fori_loop(8, 64, step_two(sides2b), none, unroll=UNROLL)
    lane16 = lax.broadcasted_iota(jnp.int32, (16, 128), 1)
    row16 = lax.broadcasted_iota(jnp.int32, (16, 128), 0)
    zbuf[lon] = jnp.where(lane16 < 64, sums[0:16], pltpu.roll(sums[16:32], 64, 1))
    kw = take(zbuf.at[0:15])
    for i in range(1, 16):
        send(zbuf.at[lon], zbuf.at[lon], (lat, wrap(lon + i, 16)), kw)
    mark("s20_pump")
    pump("c", 6)
    pump("a", 3)
    pump("b", 7)
    pump("c", 7)
    mark("s22_pump")
    mark("s23_xwait")
    arrived(xbuf.at[0:15], kx)
    mark("s24_turn")
    got = jnp.concatenate([xbuf[i] for i in range(16)], axis=0)
    turned = jnp.zeros((16, 128), F32)
    group = lane16 // 8
    for d in range(16):
        moved = got if d == 0 else pltpu.roll(pltpu.roll(got, 16 - d, 0), 8 * d, 1)
        turned = jnp.where(lax.rem(group - row16 + 16, 16) == d, moved, turned)
    for i in range(16):
        ybuf[i] = turned[i:i + 1, :]
    obuf[lat] = ybuf[lat]
    ky = take(obuf.at[0:15])
    for i in range(1, 16):
        to = wrap(lat + i, 16)
        send(ybuf.at[to], obuf.at[lat], (to, lon), ky)
    mark("s25_pump")
    pump("a", 4)
    pump("b", 8)
    pump("c", 8)
    pump("b", 9)
    mark("s21_rest")
    arrived(zbuf.at[0:15], kw)
    total = zbuf[0]
    for i in range(1, 16):
        total = total + zbuf[i]
    total = total * (1.0 / 2048.0)
    mean = jnp.concatenate([total, pltpu.roll(total, 64, 1)], axis=0)

    def rest(j, carry):
        filtered(j, mean)
        return carry

    lax.fori_loop(8, 64, rest, 0, unroll=UNROLL)
    out_field = load(aout, aout_h, 18)
    mark("s26_owait")
    pump("a", 5)
    pump("c", 9)
    pump("b", 10)
    pump("b", 11)
    arrived(obuf.at[0:15], ky)

    mark("s27_fresh")
    packed = jnp.zeros((8, 128), F32)
    for v in range(8):
        f = jnp.zeros((8, 128), F32)
        for a in range(16):
            f = f + jnp.where(reg[a:a + 1, :] == row8 + 8 * v, obuf[a], 0.0)
        for shift in (64, 32, 16, 8):
            f = f + pltpu.roll(f, shift, 1)
        packed = jnp.where(lane8 // 8 == v, f, packed)
    packed = packed.astype(BF16).astype(F32)
    fr[y, xl, z, xh] = (packed[0:4] + pltpu.roll(packed[4:8], 64, 1)).astype(BF16)
    kf = take(fr.at[0:3, 0, 0:5, 0])
    for i in range(1, 16):
        here = fr.at[y, xl, z, xh]
        send(here, here, (lat, wrap(lon + i, 16)), kf)
    mark("s28_pump")
    pump("a", 6)
    pump("c", 10)
    pump("b", 12)
    pump("b", 13)
    mark("s29_fwait")
    arrived(fr.at[0:3, 0, 0:5, 0], kf)
    kg = take(fr.at[:, :, 0:7])
    for i in range(1, 8):
        g = wrap(lat // 2 + i, 8)
        send(fr.at[y, xl], fr.at[y, xl], (g * 2 + core, lon), kg)
    mark("s30_pump")
    pump("a", 7)
    pump("c", 11)
    pump("b", 14)
    pltpu.make_async_copy(cmat.at[:, 0:64], cmat.at[:, 0:64], lsem.at[0]).wait()
    arrived(cmat.at[:, 0:64], k_cov)

    mark("s31_product")
    pacc[...] = jnp.zeros((2, 64, 512), F32)

    def product(g, carry):
        gy, gx = g // 2, lax.rem(g, 2)
        c = cmat[g]
        r0 = jnp.concatenate(
            [b0[gy, gx][:, :, 0:64].reshape(1024, 128), b1[gy, gx].reshape(1024, 128)], axis=1
        )
        left = dot(c, r0)
        pacc[0, :, 0:256] += left[0:64]
        pacc[1, :, 0:256] += left[64:128]
        tails = b0[gy, gx][:, :, 64:80].reshape(256, 128)
        pieces = []
        for q in range(4):
            sel = (
                lax.broadcasted_iota(jnp.int32, (128, 128), 0)
                == lax.broadcasted_iota(jnp.int32, (128, 128), 1) + 32 * q
            ).astype(F32).astype(BF16)
            pieces.append(dot(tails, sel).astype(BF16).reshape(16, 16, 128))
        last = jnp.concatenate(pieces, axis=1).reshape(1024, 128)
        right = dot(c, jnp.concatenate([b2[gy, gx].reshape(1024, 128), last], axis=1))
        pacc[0, :, 256:512] += right[0:64]
        pacc[1, :, 256:512] += right[64:128]
        return carry

    lax.fori_loop(0, 8, product, 0, unroll=2)
    kp = take(precv)
    send(pacc.at[1 - core], precv, other, kp)

    mark("s32_f2wait")
    arrived(fr.at[:, :, 0:7], kg)

    mark("s33_freshprod")

    def fresh_product(g, acc):
        f = fr[g // 2, lax.rem(g, 2)].reshape(16, 4, 128).astype(F32)
        f = jnp.concatenate([f, f], axis=1)
        lanes = (
            lax.broadcasted_iota(jnp.int32, (16, 8, 128), 2) // 8
            - lax.broadcasted_iota(jnp.int32, (16, 8, 128), 1) // 4 * 8
        )
        w = jnp.concatenate([jnp.where(lanes == v, f, 0.0) for v in range(8)], axis=1)
        return acc + dot(cmat[g], w.astype(BF16).reshape(1024, 128))

    added = lax.fori_loop(0, 8, fresh_product, jnp.zeros((128, 128), F32), unroll=2)
    for shift in (64, 32, 16, 8):
        added = added + pltpu.roll(added, shift, 1)
    aacc[0] = added[0:64]
    aacc[1] = added[64:128]
    mark("s34_exch")
    ka = take(arecv)
    send(aacc.at[1 - core], arecv, other, ka)
    arrived(precv, kp)
    arrived(arecv, ka)
    mark("s35_final")
    mine = aacc[core] + arecv[...]
    base = pacc[core] + precv[...]
    for n in range(4):
        week_of = (lax.broadcasted_iota(jnp.int32, (64, 128), 1) + 128 * n) // 8
        pre[:, 128 * n:128 * n + 128] = base[:, 128 * n:128 * n + 128] + jnp.where(
            week_of == jnp.broadcast_to(week[...], (64, 128)), mine, 0.0
        )
    out_pre = load(pre, pre_h, 19)
    for view, k in sends:
        remote(view, view, (lat, lon), k).wait_send()
    out_field.wait()
    out_pre.wait()
    mark("")


def finish(field, wide, aout, pre, held, block, trimmed, sem):
    reads = [pltpu.make_async_copy(field.at[t], held.at[t], sem.at[t]) for t in range(8)]
    small = pltpu.make_async_copy(wide, block, sem.at[8])
    small.start()
    for c in reads:
        c.start()
    small.wait()
    trimmed[...] = block[:, 0:416]
    writes = [pltpu.make_async_copy(trimmed, pre, sem.at[9])]
    writes[0].start()
    for t in range(8):
        reads[t].wait()
        c = pltpu.make_async_copy(held.at[t], aout.at[t], sem.at[10 + t])
        c.start()
        writes.append(c)
    for c in writes:
        c.wait()


COPIES = 64
UNROLL = 4
PROFILE = False


def shards(adjoint, transport, cell_weight, region_local, tile_regions, polar_rows, week_index, grad_in, covariance):
    hbm = pl.BlockSpec(memory_space=pl.ANY)
    aout, pre = pl.pallas_call(
        kernel,
        out_shape=(
            jax.ShapeDtypeStruct((8, 8, 32, 128), F32),
            jax.ShapeDtypeStruct((64, 512), F32),
        ),
        in_specs=[hbm] * 9,
        out_specs=(hbm, hbm),
        scratch_shapes=[
            pltpu.VMEM((8, 8, 32, 128), F32),
            pltpu.VMEM((6, 8, 32, 128), F32),
            pltpu.VMEM((32, 128), F32),
            pltpu.VMEM((32, 128), jnp.int32),
            pltpu.VMEM((256, 128), jnp.int32),
            pltpu.VMEM((1, 32), jnp.int32),
            pltpu.VMEM((1, 1), jnp.int32),
            pltpu.VMEM((64, 416), BF16),
            pltpu.VMEM((8, 8, 32, 128), F32),
            pltpu.VMEM((8, 32, 128), F32),
            pltpu.VMEM((4, 2, 8, 2, 80, 128), BF16),
            pltpu.VMEM((4, 2, 8, 2, 64, 128), BF16),
            pltpu.VMEM((4, 2, 8, 2, 64, 128), BF16),
            pltpu.VMEM((8, 128, 1024), BF16),
            pltpu.VMEM((4, 2, 8, 2, 4, 128), BF16),
            pltpu.VMEM((4, 32, 128), F32),
            pltpu.VMEM((2, 64, 128), F32),
            pltpu.VMEM((2, 64, 128), F32),
            pltpu.VMEM((4, 32, 128), F32),
            pltpu.VMEM((4, 32, 128), F32),
            pltpu.VMEM((2, 64, 128), F32),
            pltpu.VMEM((2, 64, 128), F32),
            pltpu.VMEM((16, 16, 128), F32),
            pltpu.VMEM((16, 8, 128), F32),
            pltpu.VMEM((16, 1, 128), F32),
            pltpu.VMEM((16, 1, 128), F32),
            pltpu.VMEM((16, 1, 128), F32),
            pltpu.VMEM((16, 1, 128), F32),
            pltpu.VMEM((2, 64, 512), F32),
            pltpu.VMEM((64, 512), F32),
            pltpu.VMEM((2, 64, 128), F32),
            pltpu.VMEM((64, 128), F32),
            pltpu.VMEM((8, 8, 32, 128), F32),
            pltpu.VMEM((64, 512), F32),
            pltpu.SemaphoreType.DMA((COPIES,)),
            pltpu.SemaphoreType.DMA((COPIES,)),
            pltpu.SemaphoreType.DMA((1,)),
            pltpu.SemaphoreType.DMA((20,)),
        ],
        compiler_params=pltpu.CompilerParams(
            collective_id=0, has_side_effects=True, vmem_limit_bytes=67043328
        ),
        name="window",
    )(
        adjoint, transport, cell_weight, region_local, tile_regions,
        polar_rows.reshape(1, 32), week_index.reshape(1, 1), grad_in, covariance,
    )
    return pl.pallas_call(
        finish,
        out_shape=(
            jax.ShapeDtypeStruct((8, 8, 32, 128), F32),
            jax.ShapeDtypeStruct((64, 416), F32),
        ),
        in_specs=[hbm] * 2,
        out_specs=(hbm, hbm),
        scratch_shapes=[
            pltpu.VMEM((8, 8, 32, 128), F32),
            pltpu.VMEM((64, 512), F32),
            pltpu.VMEM((64, 416), F32),
            pltpu.SemaphoreType.DMA((18,)),
        ],
        compiler_params=pltpu.CompilerParams(vmem_limit_bytes=67043328),
        name="finish",
    )(aout, pre)


def solution(mesh):
    both = ("lat", "lon")
    return jax.shard_map(
        shards,
        mesh=mesh,
        in_specs=(
            P(None, None, "lat", "lon"), P(None, None, "lat", "lon"), P("lat", "lon"), P("lat", "lon"),
            P(), P("lat"), P(), P(both, None), P(both, None),
        ),
        out_specs=(P(None, None, "lat", "lon"), P(both, None)),
        check_vma=False,
    )
```

```python
import functools

import jax
import jax.numpy as jnp
from jax import lax
from jax.experimental import pallas as pl
from jax.experimental.pallas import tpu as pltpu
from jax.sharding import PartitionSpec as P

MESH = pl.DeviceIdType.MESH
F32 = jnp.float32
BF16 = jnp.bfloat16
ALL = slice(None)


def dot(a, b):
    return lax.dot_general(a, b, (((1,), (0,)), ((), ())), preferred_element_type=F32)


def dot_nt(a, b):
    return lax.dot_general(a, b, (((1,), (1,)), ((), ())), preferred_element_type=F32)


def kernel(
    adj_h, tr_h, weight_h, rl_h, tiles_h, polar_h, week_h, grad, cov,
    aout_h, pre_h,
    adj, tr, weight, rl, tiles, polar, week, gtail,
    first, surf, b0, b1, b2, cmat, fr, col_s, row_n, row_s, col_e, col_w, halo_n, halo_s,
    zbuf, ybar, mbuf, xbuf, ybuf, obuf, pacc, precv, aacc, arecv,
    aout, pre, ssem, rsem, lsem, insem,
):
    lat = lax.axis_index("lat")
    lon = lax.axis_index("lon")
    core = lax.rem(lat, 2)
    xl = lax.rem(lat // 2, 2)
    y = lat // 4
    z = lon // 2
    xh = lax.rem(lon, 2)
    x = xh * 2 + xl
    me = {"x": x, "y": y, "z": z}
    size = {"x": 4, "y": 4, "z": 8}
    counter = [0]
    sends = []

    def wrap(v, n):
        return lax.rem(v + 2 * n, n)

    def device(c, at_core):
        return ((c["y"] * 2 + lax.rem(c["x"], 2)) * 2 + at_core, c["z"] * 2 + c["x"] // 2)

    def remote(src, dst, to, k):
        return pltpu.make_async_remote_copy(
            src_ref=src, dst_ref=dst, send_sem=ssem.at[k], recv_sem=rsem.at[k],
            device_id=to, device_id_type=MESH,
        )

    def send(src, dst, to, k):
        remote(src, dst, to, k).start()

    def take(*sizes):
        k = counter[0]
        counter[0] += len(sizes)
        for i, view in enumerate(sizes):
            sends.append((view, k + i))
        return k

    def arrived(view, k):
        remote(view, view, (lat, lon), k).wait_recv()

    other = (lat + 1 - 2 * core, lon)

    cur = [None]

    def mark(n):
        if PROFILE:
            if cur[0] is not None:
                cur[0].__exit__(None, None, None)
            cur[0] = jax.named_scope(n) if n else None
            if n:
                cur[0].__enter__()

    mark("s00_entry")
    barrier = pltpu.get_barrier_semaphore()
    for k in range(1, 16):
        pl.semaphore_signal(barrier, inc=1, device_id=(lat, wrap(lon + k, 16)), device_id_type=MESH)
        pl.semaphore_signal(barrier, inc=1, device_id=(wrap(lat + k, 16), lon), device_id_type=MESH)
    pl.semaphore_signal(
        barrier, inc=1, device_id=(lat + 2 - 4 * xl, lon + 1 - 2 * xh), device_id_type=MESH
    )

    def load(src, dst, k):
        c = pltpu.make_async_copy(src, dst, insem.at[k])
        c.start()
        return c

    in_adj = [load(adj_h.at[:, l], adj.at[l], l) for l in range(8)]
    in_grad = [
        load(grad.at[:, 0:128], b0.at[y, xl, z, xh, 0:64], 8),
        load(grad.at[:, 128:256], b1.at[y, xl, z, xh], 9),
        load(grad.at[:, 256:384], b2.at[y, xl, z, xh], 10),
        load(grad, gtail, 11),
    ]
    in_tr = load(tr_h, tr, 12)
    number = lat * 16 + lon
    lanes_at = pl.multiple_of(number // 128 * 128, 128)
    in_late = [
        load(weight_h, weight, 13), load(rl_h, rl, 14), load(polar_h, polar, 15),
        load(tiles_h.at[:, pl.ds(lanes_at, 128)], tiles, 16), load(week_h, week, 17),
    ]
    for g in range(8):
        c = pltpu.make_async_copy(
            cov.at[:, pl.ds(pl.multiple_of((g * 2 + core) * 1024, 1024), 1024)],
            cmat.at[g, pl.ds(pl.multiple_of(core * 64, 64), 64), :],
            lsem.at[0],
        )
        c.start()

    lane = lax.broadcasted_iota(jnp.int32, (32, 128), 1)
    row = lax.broadcasted_iota(jnp.int32, (32, 128), 0)

    def edges(step, j, v, acc):
        row_n[step, pl.ds(j, 1), :] = v[31:32, :]
        row_s[step, pl.ds(j, 1), :] = v[0:1, :]
        return jnp.where(lane // 2 == j, pltpu.roll(v, lax.rem(2 * j + 1, 128), 1), acc)

    def pack(j, acc):
        return edges(0, j, adj[j // 8, lax.rem(j, 8)], acc)

    none = jnp.zeros((32, 128), F32)
    in_adj[0].wait()
    in_adj[1].wait()
    col_s[0] = lax.fori_loop(0, 16, pack, none, unroll=4)
    mark("s01_barrier")
    pl.semaphore_wait(barrier, 31)
    mark("s02_send1")

    east, west = wrap(lon + 1, 16), wrap(lon - 1, 16)
    north, south = wrap(lat + 1, 16), wrap(lat - 1, 16)

    def halo_send(s, i, lo, hi):
        rows = pl.ds(lo, hi - lo)
        cols = col_s.at[2 * s + i]
        k = take(cols, cols, row_n.at[s, rows], row_n.at[s, rows])
        send(row_n.at[s, rows], halo_s.at[s, rows], (north, lon), k + 2)
        send(row_s.at[s, rows], halo_n.at[s, rows], (south, lon), k + 3)
        send(col_s.at[2 * s + i], col_w.at[2 * s + i], (lat, east), k)
        send(col_s.at[2 * s + i], col_e.at[2 * s + i], (lat, west), k + 1)
        return k

    def halo_wait(s, i, lo, hi, k):
        rows = pl.ds(lo, hi - lo)
        arrived(col_w.at[2 * s + i], k)
        arrived(col_e.at[2 * s + i], k + 1)
        arrived(halo_s.at[s, rows], k + 2)
        arrived(halo_n.at[s, rows], k + 3)
        return jnp.where(lax.rem(lane, 2) == 1, col_e[2 * s + i], pltpu.roll(col_w[2 * s + i], 2, 1))

    parts = {
        "a": (b0, "zyx", 48),
        "b": (b1, "yxz", 32),
        "c": (b2, "xzy", 32),
    }

    def slot(buf, at, rows):
        yi = at["y"] if at["y"] is not None else ALL
        zi = at["z"] if at["z"] is not None else ALL
        if at["x"] is None:
            return buf.at[yi, :, zi, :, rows]
        return buf.at[yi, lax.rem(at["x"], 2), zi, at["x"] // 2, rows]

    def whole(buf):
        return pl.ds(0, buf.shape[4])

    ids = {}

    singles = {"a": b0.at[0, 0, 0:7, 0], "b": b1.at[0:3, 0, 0, 0], "c": b2.at[0, 0, 0:3, 0]}
    views = {
        "a": {1: b0.at[0, 0, :, 0], 2: b0.at[0, 0], 4: b0.at[0]},
        "b": {1: b1.at[:, 0, 0, 0], 2: b1.at[:, 0, 0], 4: b1.at[:, :, 0]},
        "c": {1: b2.at[0, :, 0], 2: b2.at[0, 0, 0:4], 4: b2.at[0, 0]},
    }

    def direct_start(p):
        buf, order, _ = parts[p]
        d = order[0]
        n = size[d]
        k = take(singles[p])
        ids[p, 1] = k
        for i in range(1, n):
            to = dict(me)
            to[d] = wrap(me[d] + i, n)
            here = slot(buf, me, whole(buf))
            send(here, here, device(to, core), k)

    def direct_wait(p):
        arrived(singles[p], ids[p, 1])

    groups = {4: ((0,), (1, 3), (2,)), 8: ((0,), (1, 7), (2, 6), (3, 5), (4,))}

    def offsets(p, stage, g):
        return groups[size[parts[p][1][1]]][g] if stage == 3 else (0,)

    def unit(p, stage, s, g):
        n = size[parts[p][1][stage - 1]]
        return views[p][len(offsets(p, stage, g)) * (1 if s == n // 2 else 2)]

    def ring(p, stage, s, off):
        buf, order, half = parts[p]
        d = order[stage - 1]
        n = size[d]
        at = {c: (None if c in order[:stage - 1] else me[c]) for c in "xyz"}
        if stage == 3:
            at[order[1]] = wrap(me[order[1]] + off, size[order[1]])
        last = s == n // 2
        rows_r = pl.ds(0, half) if last else whole(buf)
        rows_l = pl.ds(half, buf.shape[4] - half) if last else whole(buf)
        return buf, d, n, at, rows_r, rows_l

    def ring_start(p, stage, s, g):
        k = take(unit(p, stage, s, g))
        ids[p, stage, s, g] = k
        for off in offsets(p, stage, g):
            buf, d, n, at, rows_r, rows_l = ring(p, stage, s, off)
            right, left = dict(me), dict(me)
            right[d] = wrap(me[d] + 1, n)
            left[d] = wrap(me[d] - 1, n)
            fwd, back = dict(at), dict(at)
            fwd[d] = wrap(me[d] - (s - 1), n)
            back[d] = wrap(me[d] + (s - 1), n)
            src = slot(buf, fwd, rows_r)
            send(src, src, device(right, core), k)
            src = slot(buf, back, rows_l)
            send(src, src, device(left, core), k)

    def ring_wait(p, stage, s, g):
        arrived(unit(p, stage, s, g), ids[p, stage, s, g])

    short = (
        ((), ((2, 1, 0), (3, 1, 0))),
        (((2, 1, 0),), ((2, 2, 0), (3, 1, 1))),
        (((3, 1, 0),), ((3, 2, 0),)),
        (((2, 2, 0),), ((3, 1, 2),)),
        (((3, 1, 1),), ((3, 2, 1),)),
        (((3, 1, 2),), ((3, 2, 2),)),
        (((3, 2, 0), (3, 2, 1), (3, 2, 2)), ()),
    )
    long = (
        ((), ((2, 1, 0),)),
        (((2, 1, 0),), ((2, 2, 0),)),
        ((), ((3, 1, 0), (3, 1, 1))),
        (((2, 2, 0),), ((3, 1, 2),)),
        (((3, 1, 0),), ((3, 2, 0),)),
        (((3, 1, 1),), ((3, 2, 1),)),
        (((3, 2, 0),), ((3, 3, 0),)),
        (((3, 1, 2),), ((3, 2, 2),)),
        (((3, 2, 1),), ((3, 3, 1),)),
        (((3, 3, 0),), ((3, 4, 0),)),
        (((3, 2, 2),), ((3, 3, 2),)),
        (((3, 3, 1),), ((3, 4, 1),)),
        (((3, 3, 2),), ((3, 4, 2),)),
        (((3, 4, 0), (3, 4, 1), (3, 4, 2)), ()),
    )
    other_way = (
        ((), ((2, 1, 0), (3, 1, 0))),
        (((2, 1, 0),), ((2, 2, 0), (3, 1, 1))),
        (((3, 1, 0),), ((3, 2, 0),)),
        (((2, 2, 0),), ((2, 3, 0), (3, 1, 2))),
        (((3, 1, 1),), ((3, 2, 1),)),
        (((2, 3, 0),), ((2, 4, 0), (3, 1, 3))),
        (((3, 1, 2),), ((3, 2, 2),)),
        (((2, 4, 0),), ((3, 1, 4),)),
        (((3, 1, 3),), ((3, 2, 3),)),
        (((3, 1, 4),), ((3, 2, 4),)),
        (((3, 2, 0), (3, 2, 1), (3, 2, 2), (3, 2, 3), (3, 2, 4)), ()),
    )
    plan = {"a": short, "b": long, "c": other_way}

    def pump(p, *events):
        for i in events:
            waits, starts = plan[p][i - 1]
            if i == 1:
                direct_wait(p)
            for w in waits:
                ring_wait(p, *w)
            for w in starts:
                ring_start(p, *w)

    k1a = halo_send(0, 0, 0, 16)
    for c in in_adj[2:]:
        c.wait()
    col_s[1] = lax.fori_loop(16, 64, pack, none, unroll=4)

    for c in in_grad:
        c.wait()
    tail = jnp.zeros((16, 128), F32)
    for q in range(4):
        sel = (
            lax.broadcasted_iota(jnp.int32, (32, 128), 1)
            == lax.broadcasted_iota(jnp.int32, (32, 128), 0) + 32 * q
        ).astype(F32).astype(BF16)
        tail = tail + dot(gtail[16 * q:16 * q + 16, 384:416], sel)
    b0[y, xl, z, xh, 64:80, :] = tail.astype(BF16)

    k1b = halo_send(0, 1, 16, 64)
    for p in "bac":
        direct_start(p)
    k_cov = take(cmat.at[:, 0:64])
    for g in range(8):
        send(
            cov.at[:, pl.ds(pl.multiple_of((g * 2 + 1 - core) * 1024, 1024), 1024)],
            cmat.at[g, pl.ds(pl.multiple_of(core * 64, 64), 64), :],
            other, k_cov,
        )

    has_north = (lat < 15).astype(F32)
    has_south = (lat > 0).astype(F32)

    def stencil(src, step, j, sides):
        l, t = j // 8, lax.rem(j, 8)
        c = src[l, t]
        h = pltpu.roll(sides, 126 - 2 * j, 1)
        e = jnp.where(lane == 127, h, pltpu.roll(c, 127, 1))
        v = jnp.where(lane == 0, h, pltpu.roll(c, 1, 1))
        n = jnp.where(row == 31, has_north * halo_n[step, pl.ds(j, 1), :], pltpu.roll(c, 31, 0))
        s = jnp.where(row == 0, has_south * halo_s[step, pl.ds(j, 1), :], pltpu.roll(c, 1, 0))
        u = src[jnp.minimum(l + 1, 7), t]
        d = src[jnp.maximum(l - 1, 0), t]
        return (
            c + tr[0, l] * (e - c) + tr[1, l] * (v - c) + tr[2, l] * (n - c)
            + tr[3, l] * (s - c) + tr[4, l] * (u - c) + tr[5, l] * (d - c)
        )

    mark("s03_halo1a")
    in_tr.wait()
    sides1a = halo_wait(0, 0, 0, 16, k1a)
    mark("s04_step1a")

    def step_one(sides):
        def body(j, acc):
            v = stencil(adj, 0, j, sides)
            first[j // 8, lax.rem(j, 8)] = v
            return edges(1, j, v, acc)
        return body

    col_s[2] = lax.fori_loop(0, 8, step_one(sides1a), none, unroll=UNROLL)
    k2a = halo_send(1, 0, 0, 8)
    mark("s05_step1a2")
    rest1 = lax.fori_loop(8, 16, step_one(sides1a), none, unroll=UNROLL)
    mark("s06_pump")
    pump("b", 1)
    pump("c", 1)
    mark("s07_halo1b")
    sides1b = halo_wait(0, 1, 16, 64, k1b)
    mark("s08_step1b")
    col_s[3] = lax.fori_loop(16, 64, step_one(sides1b), rest1, unroll=UNROLL)
    k2b = halo_send(1, 1, 8, 64)
    mark("s09_pump")
    mark("s10_halo2a")
    sides2a = halo_wait(1, 0, 0, 8, k2a)
    mark("s11_step2a")

    def step_two(sides):
        def body(j, acc):
            v = stencil(first, 1, j, sides)
            aout[lax.rem(j, 8), j // 8] = v
            return jnp.where(lane == j, jnp.sum(v, axis=1, keepdims=True), acc)
        return body

    sums = lax.fori_loop(0, 8, step_two(sides2a), none, unroll=UNROLL)
    lane8 = lax.broadcasted_iota(jnp.int32, (8, 128), 1)
    row8 = lax.broadcasted_iota(jnp.int32, (8, 128), 0)
    tight = sums[0:8]
    for i in range(1, 4):
        tight = jnp.where(lane8 // 8 == i, pltpu.roll(sums[8 * i:8 * i + 8], 8 * i, 1), tight)
    ybar[lon] = tight
    kz = take(ybar.at[0:15])
    for i in range(1, 16):
        send(ybar.at[lon], ybar.at[lon], (lat, wrap(lon + i, 16)), kz)
    mark("s12_pump")
    pump("b", 2)
    pump("c", 2)
    pump("b", 3)
    pump("a", 1)
    pump("c", 3)
    pump("b", 4)
    mark("s15_pump")
    for c in in_late:
        c.wait()
    flags = 0.5 * jnp.sum(
        jnp.where(
            lax.broadcasted_iota(jnp.int32, (32, 32), 0) == lax.broadcasted_iota(jnp.int32, (32, 32), 1),
            jnp.broadcast_to(polar[...], (32, 32)), 0,
        ).astype(F32), axis=1, keepdims=True
    )
    lane256 = lax.broadcasted_iota(jnp.int32, (256, 128), 1)
    row256 = lax.broadcasted_iota(jnp.int32, (256, 128), 0)
    mine_at = jnp.sum(
        jnp.where(lane256 == number - lanes_at, tiles[...] - 64 * number, 0).astype(F32), axis=1, keepdims=True
    )
    spread = jnp.where(lane256 // 8 == lax.rem(row256, 16), mine_at, 0.0).astype(BF16)
    pick = (
        lax.broadcasted_iota(jnp.int32, (16, 256), 1) // 16 == lax.broadcasted_iota(jnp.int32, (16, 256), 0)
    ).astype(F32).astype(BF16)
    reg = dot(pick, spread).astype(jnp.int32)
    mark("s16_zwait")
    arrived(ybar.at[0:15], kz)
    mark("s17_surf")
    total = ybar[0]
    for i in range(1, 16):
        total = total + ybar[i]
    total = total * (1.0 / 2048.0)
    mean0 = jnp.concatenate([total] + [pltpu.roll(total, 128 - 8 * i, 1) for i in range(1, 4)], axis=0)

    def filtered(j, mean):
        v = aout[lax.rem(j, 8), j // 8]
        v = v + flags * (jnp.sum(jnp.where(lane == j, mean, 0.0), axis=1, keepdims=True) - v)
        aout[lax.rem(j, 8), j // 8] = v
        return v

    for t in range(8):
        surf[t] = filtered(t, mean0) * weight[...]

    mark("s18_pump")
    pump("c", 4)
    mark("s19_regions")

    sub8 = lax.broadcasted_iota(jnp.int32, (16, 128), 0)

    def regions(r, acc):
        lhs, rhs = [], [[], [], []]
        for h in range(2):
            i = 2 * r + h
            local = rl[pl.ds(i, 1), :]
            low = jnp.broadcast_to(local & 15, (16, 128))
            high = jnp.broadcast_to(local >> 4, (8, 128))
            lhs.append((low == sub8).astype(F32).astype(BF16))
            s = jnp.concatenate([surf[t, pl.ds(i, 1), :] for t in range(8)], axis=0)
            for n in range(3):
                piece = s.astype(BF16).astype(F32)
                s = s - piece
                rhs[n].append(
                    jnp.concatenate([jnp.where(high == a, piece, 0.0) for a in range(16)], axis=0).astype(BF16)
                )
        left = jnp.concatenate(lhs, axis=1)
        for n in range(3):
            acc = acc + dot_nt(left, jnp.concatenate(rhs[n], axis=1))
        return acc

    m = lax.fori_loop(0, 16, regions, jnp.zeros((16, 128), F32), unroll=4)
    for i in range(16):
        mbuf[i] = m[i:i + 1, :]
    xbuf[lon] = mbuf[lon]
    kx = take(xbuf.at[0:15])
    for i in range(1, 16):
        to = wrap(lon + i, 16)
        send(mbuf.at[to], xbuf.at[lon], (lat, to), kx)

    mark("s13_halo2b")
    pump("a", 2)
    pump("b", 5)
    pump("c", 5)
    pump("b", 6)
    sides2b = halo_wait(1, 1, 8, 64, k2b)
    mark("s14_step2b")
    sums = lax.fori_loop(8, 64, step_two(sides2b), none, unroll=UNROLL)
    lane16 = lax.broadcasted_iota(jnp.int32, (16, 128), 1)
    row16 = lax.broadcasted_iota(jnp.int32, (16, 128), 0)
    zbuf[lon] = jnp.where(lane16 < 64, sums[0:16], pltpu.roll(sums[16:32], 64, 1))
    kw = take(zbuf.at[0:15])
    for i in range(1, 16):
        send(zbuf.at[lon], zbuf.at[lon], (lat, wrap(lon + i, 16)), kw)
    mark("s20_pump")
    pump("c", 6)
    pump("a", 3)
    pump("b", 7)
    pump("c", 7)
    mark("s22_pump")
    mark("s23_xwait")
    arrived(xbuf.at[0:15], kx)
    mark("s24_turn")
    got = jnp.concatenate([xbuf[i] for i in range(16)], axis=0)
    turned = jnp.zeros((16, 128), F32)
    group = lane16 // 8
    for d in range(16):
        moved = got if d == 0 else pltpu.roll(pltpu.roll(got, 16 - d, 0), 8 * d, 1)
        turned = jnp.where(lax.rem(group - row16 + 16, 16) == d, moved, turned)
    for i in range(16):
        ybuf[i] = turned[i:i + 1, :]
    obuf[lat] = ybuf[lat]
    ky = take(obuf.at[0:15])
    for i in range(1, 16):
        to = wrap(lat + i, 16)
        send(ybuf.at[to], obuf.at[lat], (to, lon), ky)
    mark("s25_pump")
    pump("a", 4)
    pump("b", 8)
    pump("c", 8)
    pump("b", 9)
    mark("s21_rest")
    arrived(zbuf.at[0:15], kw)
    total = zbuf[0]
    for i in range(1, 16):
        total = total + zbuf[i]
    total = total * (1.0 / 2048.0)
    mean = jnp.concatenate([total, pltpu.roll(total, 64, 1)], axis=0)

    def rest(j, carry):
        filtered(j, mean)
        return carry

    lax.fori_loop(8, 64, rest, 0, unroll=UNROLL)
    out_field = load(aout, aout_h, 18)
    mark("s26_owait")
    pump("a", 5)
    pump("c", 9)
    pump("b", 10)
    pump("b", 11)
    arrived(obuf.at[0:15], ky)

    mark("s27_fresh")
    packed = jnp.zeros((8, 128), F32)
    for v in range(8):
        f = jnp.zeros((8, 128), F32)
        for a in range(16):
            f = f + jnp.where(reg[a:a + 1, :] == row8 + 8 * v, obuf[a], 0.0)
        for shift in (64, 32, 16, 8):
            f = f + pltpu.roll(f, shift, 1)
        packed = jnp.where(lane8 // 8 == v, f, packed)
    packed = packed.astype(BF16).astype(F32)
    fr[y, xl, z, xh] = (packed[0:4] + pltpu.roll(packed[4:8], 64, 1)).astype(BF16)
    kf = take(fr.at[0:3, 0, 0:5, 0])
    for i in range(1, 16):
        here = fr.at[y, xl, z, xh]
        send(here, here, (lat, wrap(lon + i, 16)), kf)
    mark("s28_pump")
    pump("a", 6)
    pump("c", 10)
    pump("b", 12)
    pump("b", 13)
    mark("s29_fwait")
    arrived(fr.at[0:3, 0, 0:5, 0], kf)
    kg = take(fr.at[:, :, 0:7])
    for i in range(1, 8):
        g = wrap(lat // 2 + i, 8)
        send(fr.at[y, xl], fr.at[y, xl], (g * 2 + core, lon), kg)
    mark("s30_pump")
    pump("a", 7)
    pump("c", 11)
    pump("b", 14)
    pltpu.make_async_copy(cmat.at[:, 0:64], cmat.at[:, 0:64], lsem.at[0]).wait()
    arrived(cmat.at[:, 0:64], k_cov)

    mark("s31_product")
    pacc[...] = jnp.zeros((2, 64, 512), F32)

    def product(g, carry):
        gy, gx = g // 2, lax.rem(g, 2)
        c = cmat[g]
        r0 = jnp.concatenate(
            [b0[gy, gx][:, :, 0:64].reshape(1024, 128), b1[gy, gx].reshape(1024, 128)], axis=1
        )
        left = dot(c, r0)
        pacc[0, :, 0:256] += left[0:64]
        pacc[1, :, 0:256] += left[64:128]
        tails = b0[gy, gx][:, :, 64:80].reshape(256, 128)
        pieces = []
        for q in range(4):
            sel = (
                lax.broadcasted_iota(jnp.int32, (128, 128), 0)
                == lax.broadcasted_iota(jnp.int32, (128, 128), 1) + 32 * q
            ).astype(F32).astype(BF16)
            pieces.append(dot(tails, sel).astype(BF16).reshape(16, 16, 128))
        last = jnp.concatenate(pieces, axis=1).reshape(1024, 128)
        right = dot(c, jnp.concatenate([b2[gy, gx].reshape(1024, 128), last], axis=1))
        pacc[0, :, 256:512] += right[0:64]
        pacc[1, :, 256:512] += right[64:128]
        return carry

    lax.fori_loop(0, 8, product, 0, unroll=4)
    kp = take(precv)
    send(pacc.at[1 - core], precv, other, kp)

    mark("s32_f2wait")
    arrived(fr.at[:, :, 0:7], kg)

    mark("s33_freshprod")

    def fresh_product(g, acc):
        f = fr[g // 2, lax.rem(g, 2)].reshape(16, 4, 128).astype(F32)
        f = jnp.concatenate([f, f], axis=1)
        lanes = (
            lax.broadcasted_iota(jnp.int32, (16, 8, 128), 2) // 8
            - lax.broadcasted_iota(jnp.int32, (16, 8, 128), 1) // 4 * 8
        )
        w = jnp.concatenate([jnp.where(lanes == v, f, 0.0) for v in range(8)], axis=1)
        return acc + dot(cmat[g], w.astype(BF16).reshape(1024, 128))

    added = lax.fori_loop(0, 8, fresh_product, jnp.zeros((128, 128), F32), unroll=4)
    for shift in (64, 32, 16, 8):
        added = added + pltpu.roll(added, shift, 1)
    aacc[0] = added[0:64]
    aacc[1] = added[64:128]
    mark("s34_exch")
    ka = take(arecv)
    send(aacc.at[1 - core], arecv, other, ka)
    arrived(precv, kp)
    arrived(arecv, ka)
    mark("s35_final")
    mine = aacc[core] + arecv[...]
    base = pacc[core] + precv[...]
    for n in range(4):
        week_of = (lax.broadcasted_iota(jnp.int32, (64, 128), 1) + 128 * n) // 8
        pre[:, 128 * n:128 * n + 128] = base[:, 128 * n:128 * n + 128] + jnp.where(
            week_of == jnp.broadcast_to(week[...], (64, 128)), mine, 0.0
        )
    out_pre = load(pre, pre_h, 19)
    for view, k in sends:
        remote(view, view, (lat, lon), k).wait_send()
    out_field.wait()
    out_pre.wait()
    mark("")


def finish(field, wide, aout, pre, held, block, trimmed, sem):
    reads = [pltpu.make_async_copy(field.at[t], held.at[t], sem.at[t]) for t in range(8)]
    small = pltpu.make_async_copy(wide, block, sem.at[8])
    small.start()
    for c in reads:
        c.start()
    small.wait()
    trimmed[...] = block[:, 0:416]
    writes = [pltpu.make_async_copy(trimmed, pre, sem.at[9])]
    writes[0].start()
    for t in range(8):
        reads[t].wait()
        c = pltpu.make_async_copy(held.at[t], aout.at[t], sem.at[10 + t])
        c.start()
        writes.append(c)
    for c in writes:
        c.wait()


COPIES = 64
UNROLL = 4
PROFILE = False


def shards(adjoint, transport, cell_weight, region_local, tile_regions, polar_rows, week_index, grad_in, covariance):
    hbm = pl.BlockSpec(memory_space=pl.ANY)
    aout, pre = pl.pallas_call(
        kernel,
        out_shape=(
            jax.ShapeDtypeStruct((8, 8, 32, 128), F32),
            jax.ShapeDtypeStruct((64, 512), F32),
        ),
        in_specs=[hbm] * 9,
        out_specs=(hbm, hbm),
        scratch_shapes=[
            pltpu.VMEM((8, 8, 32, 128), F32),
            pltpu.VMEM((6, 8, 32, 128), F32),
            pltpu.VMEM((32, 128), F32),
            pltpu.VMEM((32, 128), jnp.int32),
            pltpu.VMEM((256, 128), jnp.int32),
            pltpu.VMEM((1, 32), jnp.int32),
            pltpu.VMEM((1, 1), jnp.int32),
            pltpu.VMEM((64, 416), BF16),
            pltpu.VMEM((8, 8, 32, 128), F32),
            pltpu.VMEM((8, 32, 128), F32),
            pltpu.VMEM((4, 2, 8, 2, 80, 128), BF16),
            pltpu.VMEM((4, 2, 8, 2, 64, 128), BF16),
            pltpu.VMEM((4, 2, 8, 2, 64, 128), BF16),
            pltpu.VMEM((8, 128, 1024), BF16),
            pltpu.VMEM((4, 2, 8, 2, 4, 128), BF16),
            pltpu.VMEM((4, 32, 128), F32),
            pltpu.VMEM((2, 64, 128), F32),
            pltpu.VMEM((2, 64, 128), F32),
            pltpu.VMEM((4, 32, 128), F32),
            pltpu.VMEM((4, 32, 128), F32),
            pltpu.VMEM((2, 64, 128), F32),
            pltpu.VMEM((2, 64, 128), F32),
            pltpu.VMEM((16, 16, 128), F32),
            pltpu.VMEM((16, 8, 128), F32),
            pltpu.VMEM((16, 1, 128), F32),
            pltpu.VMEM((16, 1, 128), F32),
            pltpu.VMEM((16, 1, 128), F32),
            pltpu.VMEM((16, 1, 128), F32),
            pltpu.VMEM((2, 64, 512), F32),
            pltpu.VMEM((64, 512), F32),
            pltpu.VMEM((2, 64, 128), F32),
            pltpu.VMEM((64, 128), F32),
            pltpu.VMEM((8, 8, 32, 128), F32),
            pltpu.VMEM((64, 512), F32),
            pltpu.SemaphoreType.DMA((COPIES,)),
            pltpu.SemaphoreType.DMA((COPIES,)),
            pltpu.SemaphoreType.DMA((1,)),
            pltpu.SemaphoreType.DMA((20,)),
        ],
        compiler_params=pltpu.CompilerParams(
            collective_id=0, has_side_effects=True, vmem_limit_bytes=67043328
        ),
        name="window",
    )(
        adjoint, transport, cell_weight, region_local, tile_regions,
        polar_rows.reshape(1, 32), week_index.reshape(1, 1), grad_in, covariance,
    )
    return pl.pallas_call(
        finish,
        out_shape=(
            jax.ShapeDtypeStruct((8, 8, 32, 128), F32),
            jax.ShapeDtypeStruct((64, 416), F32),
        ),
        in_specs=[hbm] * 2,
        out_specs=(hbm, hbm),
        scratch_shapes=[
            pltpu.VMEM((8, 8, 32, 128), F32),
            pltpu.VMEM((64, 512), F32),
            pltpu.VMEM((64, 416), F32),
            pltpu.SemaphoreType.DMA((18,)),
        ],
        compiler_params=pltpu.CompilerParams(vmem_limit_bytes=67043328),
        name="finish",
    )(aout, pre)


def solution(mesh):
    both = ("lat", "lon")
    return jax.shard_map(
        shards,
        mesh=mesh,
        in_specs=(
            P(None, None, "lat", "lon"), P(None, None, "lat", "lon"), P("lat", "lon"), P("lat", "lon"),
            P(), P("lat"), P(), P(both, None), P(both, None),
        ),
        out_specs=(P(None, None, "lat", "lon"), P(both, None)),
        check_vma=False,
    )
```

```python
import functools

import jax
import jax.numpy as jnp
from jax import lax
from jax.experimental import pallas as pl
from jax.experimental.pallas import tpu as pltpu
from jax.sharding import PartitionSpec as P

MESH = pl.DeviceIdType.MESH
F32 = jnp.float32
BF16 = jnp.bfloat16
ALL = slice(None)


def dot(a, b):
    return lax.dot_general(a, b, (((1,), (0,)), ((), ())), preferred_element_type=F32)


def dot_nt(a, b):
    return lax.dot_general(a, b, (((1,), (1,)), ((), ())), preferred_element_type=F32)


def kernel(
    adj_h, tr_h, weight_h, rl_h, tiles_h, polar_h, week_h, grad, cov,
    aout_h, pre_h,
    adj, tr, weight, rl, tiles, polar, week, gtail,
    first, surf, b0, b1, b2, cmat, fr, col_s, row_n, row_s, col_e, col_w, halo_n, halo_s,
    zbuf, ybar, mbuf, xbuf, ybuf, obuf, pacc, precv, aacc, arecv,
    aout, pre, ssem, rsem, lsem, insem,
):
    lat = lax.axis_index("lat")
    lon = lax.axis_index("lon")
    core = lax.rem(lat, 2)
    xl = lax.rem(lat // 2, 2)
    y = lat // 4
    z = lon // 2
    xh = lax.rem(lon, 2)
    x = xh * 2 + xl
    me = {"x": x, "y": y, "z": z}
    size = {"x": 4, "y": 4, "z": 8}
    counter = [0]
    sends = []

    def wrap(v, n):
        return lax.rem(v + 2 * n, n)

    def device(c, at_core):
        return ((c["y"] * 2 + lax.rem(c["x"], 2)) * 2 + at_core, c["z"] * 2 + c["x"] // 2)

    def remote(src, dst, to, k):
        return pltpu.make_async_remote_copy(
            src_ref=src, dst_ref=dst, send_sem=ssem.at[k], recv_sem=rsem.at[k],
            device_id=to, device_id_type=MESH,
        )

    def send(src, dst, to, k):
        remote(src, dst, to, k).start()

    def take(*sizes):
        k = counter[0]
        counter[0] += len(sizes)
        for i, view in enumerate(sizes):
            sends.append((view, k + i))
        return k

    def arrived(view, k):
        remote(view, view, (lat, lon), k).wait_recv()

    other = (lat + 1 - 2 * core, lon)

    cur = [None]

    def mark(n):
        if PROFILE:
            if cur[0] is not None:
                cur[0].__exit__(None, None, None)
            cur[0] = jax.named_scope(n) if n else None
            if n:
                cur[0].__enter__()

    mark("s00_entry")
    barrier = pltpu.get_barrier_semaphore()
    for k in range(1, 16):
        pl.semaphore_signal(barrier, inc=1, device_id=(lat, wrap(lon + k, 16)), device_id_type=MESH)
        pl.semaphore_signal(barrier, inc=1, device_id=(wrap(lat + k, 16), lon), device_id_type=MESH)
    pl.semaphore_signal(
        barrier, inc=1, device_id=(lat + 2 - 4 * xl, lon + 1 - 2 * xh), device_id_type=MESH
    )

    def load(src, dst, k):
        c = pltpu.make_async_copy(src, dst, insem.at[k])
        c.start()
        return c

    in_adj = [load(adj_h.at[:, l], adj.at[l], l) for l in range(8)]
    in_grad = [
        load(grad.at[:, 0:128], b0.at[y, xl, z, xh, 0:64], 8),
        load(grad.at[:, 128:256], b1.at[y, xl, z, xh], 9),
        load(grad.at[:, 256:384], b2.at[y, xl, z, xh], 10),
        load(grad, gtail, 11),
    ]
    in_tr = load(tr_h, tr, 12)
    number = lat * 16 + lon
    lanes_at = pl.multiple_of(number // 128 * 128, 128)
    in_late = [
        load(weight_h, weight, 13), load(rl_h, rl, 14), load(polar_h, polar, 15),
        load(tiles_h.at[:, pl.ds(lanes_at, 128)], tiles, 16), load(week_h, week, 17),
    ]
    for g in range(8):
        c = pltpu.make_async_copy(
            cov.at[:, pl.ds(pl.multiple_of((g * 2 + core) * 1024, 1024), 1024)],
            cmat.at[g, pl.ds(pl.multiple_of(core * 64, 64), 64), :],
            lsem.at[0],
        )
        c.start()

    lane = lax.broadcasted_iota(jnp.int32, (32, 128), 1)
    row = lax.broadcasted_iota(jnp.int32, (32, 128), 0)

    def edges(step, j, v, acc):
        row_n[step, pl.ds(j, 1), :] = v[31:32, :]
        row_s[step, pl.ds(j, 1), :] = v[0:1, :]
        return jnp.where(lane // 2 == j, pltpu.roll(v, lax.rem(2 * j + 1, 128), 1), acc)

    def pack(j, acc):
        return edges(0, j, adj[j // 8, lax.rem(j, 8)], acc)

    none = jnp.zeros((32, 128), F32)
    in_adj[0].wait()
    in_adj[1].wait()
    col_s[0] = lax.fori_loop(0, 16, pack, none, unroll=4)
    mark("s01_barrier")
    pl.semaphore_wait(barrier, 31)
    mark("s02_send1")

    east, west = wrap(lon + 1, 16), wrap(lon - 1, 16)
    north, south = wrap(lat + 1, 16), wrap(lat - 1, 16)

    def halo_send(s, i, lo, hi):
        rows = pl.ds(lo, hi - lo)
        cols = col_s.at[2 * s + i]
        k = take(cols, cols, row_n.at[s, rows], row_n.at[s, rows])
        send(row_n.at[s, rows], halo_s.at[s, rows], (north, lon), k + 2)
        send(row_s.at[s, rows], halo_n.at[s, rows], (south, lon), k + 3)
        send(col_s.at[2 * s + i], col_w.at[2 * s + i], (lat, east), k)
        send(col_s.at[2 * s + i], col_e.at[2 * s + i], (lat, west), k + 1)
        return k

    def halo_wait(s, i, lo, hi, k):
        rows = pl.ds(lo, hi - lo)
        arrived(col_w.at[2 * s + i], k)
        arrived(col_e.at[2 * s + i], k + 1)
        arrived(halo_s.at[s, rows], k + 2)
        arrived(halo_n.at[s, rows], k + 3)
        return jnp.where(lax.rem(lane, 2) == 1, col_e[2 * s + i], pltpu.roll(col_w[2 * s + i], 2, 1))

    parts = {
        "a": (b0, "zyx", 48),
        "b": (b1, "yxz", 32),
        "c": (b2, "xzy", 32),
    }

    def slot(buf, at, rows):
        yi = at["y"] if at["y"] is not None else ALL
        zi = at["z"] if at["z"] is not None else ALL
        if at["x"] is None:
            return buf.at[yi, :, zi, :, rows]
        return buf.at[yi, lax.rem(at["x"], 2), zi, at["x"] // 2, rows]

    def whole(buf):
        return pl.ds(0, buf.shape[4])

    ids = {}

    singles = {"a": b0.at[0, 0, 0:7, 0], "b": b1.at[0:3, 0, 0, 0], "c": b2.at[0, 0, 0:3, 0]}
    views = {
        "a": {1: b0.at[0, 0, :, 0], 2: b0.at[0, 0], 4: b0.at[0]},
        "b": {1: b1.at[:, 0, 0, 0], 2: b1.at[:, 0, 0], 4: b1.at[:, :, 0]},
        "c": {1: b2.at[0, :, 0], 2: b2.at[0, 0, 0:4], 4: b2.at[0, 0]},
    }

    def direct_start(p):
        buf, order, _ = parts[p]
        d = order[0]
        n = size[d]
        k = take(singles[p])
        ids[p, 1] = k
        for i in range(1, n):
            to = dict(me)
            to[d] = wrap(me[d] + i, n)
            here = slot(buf, me, whole(buf))
            send(here, here, device(to, core), k)

    def direct_wait(p):
        arrived(singles[p], ids[p, 1])

    groups = {4: ((0,), (1, 3), (2,)), 8: ((0,), (1, 7), (2, 6), (3, 5), (4,))}

    def offsets(p, stage, g):
        return groups[size[parts[p][1][1]]][g] if stage == 3 else (0,)

    def unit(p, stage, s, g):
        n = size[parts[p][1][stage - 1]]
        return views[p][len(offsets(p, stage, g)) * (1 if s == n // 2 else 2)]

    def ring(p, stage, s, off):
        buf, order, half = parts[p]
        d = order[stage - 1]
        n = size[d]
        at = {c: (None if c in order[:stage - 1] else me[c]) for c in "xyz"}
        if stage == 3:
            at[order[1]] = wrap(me[order[1]] + off, size[order[1]])
        last = s == n // 2
        rows_r = pl.ds(0, half) if last else whole(buf)
        rows_l = pl.ds(half, buf.shape[4] - half) if last else whole(buf)
        return buf, d, n, at, rows_r, rows_l

    def ring_start(p, stage, s, g):
        k = take(unit(p, stage, s, g))
        ids[p, stage, s, g] = k
        for off in offsets(p, stage, g):
            buf, d, n, at, rows_r, rows_l = ring(p, stage, s, off)
            right, left = dict(me), dict(me)
            right[d] = wrap(me[d] + 1, n)
            left[d] = wrap(me[d] - 1, n)
            fwd, back = dict(at), dict(at)
            fwd[d] = wrap(me[d] - (s - 1), n)
            back[d] = wrap(me[d] + (s - 1), n)
            src = slot(buf, fwd, rows_r)
            send(src, src, device(right, core), k)
            src = slot(buf, back, rows_l)
            send(src, src, device(left, core), k)

    def ring_wait(p, stage, s, g):
        arrived(unit(p, stage, s, g), ids[p, stage, s, g])

    short = (
        ((), ((2, 1, 0), (3, 1, 0))),
        (((2, 1, 0),), ((2, 2, 0), (3, 1, 1))),
        (((3, 1, 0),), ((3, 2, 0),)),
        (((2, 2, 0),), ((3, 1, 2),)),
        (((3, 1, 1),), ((3, 2, 1),)),
        (((3, 1, 2),), ((3, 2, 2),)),
        (((3, 2, 0), (3, 2, 1), (3, 2, 2)), ()),
    )
    long = (
        ((), ((2, 1, 0),)),
        (((2, 1, 0),), ((2, 2, 0),)),
        ((), ((3, 1, 0), (3, 1, 1))),
        (((2, 2, 0),), ((3, 1, 2),)),
        (((3, 1, 0),), ((3, 2, 0),)),
        (((3, 1, 1),), ((3, 2, 1),)),
        (((3, 2, 0),), ((3, 3, 0),)),
        (((3, 1, 2),), ((3, 2, 2),)),
        (((3, 2, 1),), ((3, 3, 1),)),
        (((3, 3, 0),), ((3, 4, 0),)),
        (((3, 2, 2),), ((3, 3, 2),)),
        (((3, 3, 1),), ((3, 4, 1),)),
        (((3, 3, 2),), ((3, 4, 2),)),
        (((3, 4, 0), (3, 4, 1), (3, 4, 2)), ()),
    )
    other_way = (
        ((), ((2, 1, 0), (3, 1, 0))),
        (((2, 1, 0),), ((2, 2, 0), (3, 1, 1))),
        (((3, 1, 0),), ((3, 2, 0),)),
        (((2, 2, 0),), ((2, 3, 0), (3, 1, 2))),
        (((3, 1, 1),), ((3, 2, 1),)),
        (((2, 3, 0),), ((2, 4, 0), (3, 1, 3))),
        (((3, 1, 2),), ((3, 2, 2),)),
        (((2, 4, 0),), ((3, 1, 4),)),
        (((3, 1, 3),), ((3, 2, 3),)),
        (((3, 1, 4),), ((3, 2, 4),)),
        (((3, 2, 0), (3, 2, 1), (3, 2, 2), (3, 2, 3), (3, 2, 4)), ()),
    )
    plan = {"a": short, "b": long, "c": other_way}

    def pump(p, *events):
        for i in events:
            waits, starts = plan[p][i - 1]
            if i == 1:
                direct_wait(p)
            for w in waits:
                ring_wait(p, *w)
            for w in starts:
                ring_start(p, *w)

    k1a = halo_send(0, 0, 0, 16)
    for c in in_grad:
        c.wait()
    for p in "bc":
        direct_start(p)
    tail = jnp.zeros((16, 128), F32)
    for q in range(4):
        sel = (
            lax.broadcasted_iota(jnp.int32, (32, 128), 1)
            == lax.broadcasted_iota(jnp.int32, (32, 128), 0) + 32 * q
        ).astype(F32).astype(BF16)
        tail = tail + dot(gtail[16 * q:16 * q + 16, 384:416], sel)
    b0[y, xl, z, xh, 64:80, :] = tail.astype(BF16)

    direct_start("a")
    for c in in_adj[2:]:
        c.wait()
    col_s[1] = lax.fori_loop(16, 64, pack, none, unroll=4)

    k1b = halo_send(0, 1, 16, 64)
    k_cov = take(cmat.at[:, 0:64])
    for g in range(8):
        send(
            cov.at[:, pl.ds(pl.multiple_of((g * 2 + 1 - core) * 1024, 1024), 1024)],
            cmat.at[g, pl.ds(pl.multiple_of(core * 64, 64), 64), :],
            other, k_cov,
        )

    has_north = (lat < 15).astype(F32)
    has_south = (lat > 0).astype(F32)

    def stencil(src, step, j, sides):
        l, t = j // 8, lax.rem(j, 8)
        c = src[l, t]
        h = pltpu.roll(sides, 126 - 2 * j, 1)
        e = jnp.where(lane == 127, h, pltpu.roll(c, 127, 1))
        v = jnp.where(lane == 0, h, pltpu.roll(c, 1, 1))
        n = jnp.where(row == 31, has_north * halo_n[step, pl.ds(j, 1), :], pltpu.roll(c, 31, 0))
        s = jnp.where(row == 0, has_south * halo_s[step, pl.ds(j, 1), :], pltpu.roll(c, 1, 0))
        u = src[jnp.minimum(l + 1, 7), t]
        d = src[jnp.maximum(l - 1, 0), t]
        return (
            c + tr[0, l] * (e - c) + tr[1, l] * (v - c) + tr[2, l] * (n - c)
            + tr[3, l] * (s - c) + tr[4, l] * (u - c) + tr[5, l] * (d - c)
        )

    mark("s03_halo1a")
    in_tr.wait()
    sides1a = halo_wait(0, 0, 0, 16, k1a)
    mark("s04_step1a")

    def step_one(sides):
        def body(j, acc):
            v = stencil(adj, 0, j, sides)
            first[j // 8, lax.rem(j, 8)] = v
            return edges(1, j, v, acc)
        return body

    col_s[2] = lax.fori_loop(0, 8, step_one(sides1a), none, unroll=UNROLL)
    k2a = halo_send(1, 0, 0, 8)
    mark("s05_step1a2")
    rest1 = lax.fori_loop(8, 16, step_one(sides1a), none, unroll=UNROLL)
    mark("s06_pump")
    pump("b", 1)
    pump("c", 1)
    mark("s07_halo1b")
    sides1b = halo_wait(0, 1, 16, 64, k1b)
    mark("s08_step1b")
    col_s[3] = lax.fori_loop(16, 64, step_one(sides1b), rest1, unroll=UNROLL)
    k2b = halo_send(1, 1, 8, 64)
    mark("s09_pump")
    pump("b", 2)
    pump("c", 2)
    mark("s10_halo2a")
    sides2a = halo_wait(1, 0, 0, 8, k2a)
    mark("s11_step2a")

    def step_two(sides):
        def body(j, acc):
            v = stencil(first, 1, j, sides)
            aout[lax.rem(j, 8), j // 8] = v
            return jnp.where(lane == j, jnp.sum(v, axis=1, keepdims=True), acc)
        return body

    sums = lax.fori_loop(0, 8, step_two(sides2a), none, unroll=UNROLL)
    lane8 = lax.broadcasted_iota(jnp.int32, (8, 128), 1)
    row8 = lax.broadcasted_iota(jnp.int32, (8, 128), 0)
    tight = sums[0:8]
    for i in range(1, 4):
        tight = jnp.where(lane8 // 8 == i, pltpu.roll(sums[8 * i:8 * i + 8], 8 * i, 1), tight)
    ybar[lon] = tight
    kz = take(ybar.at[0:15])
    for i in range(1, 16):
        send(ybar.at[lon], ybar.at[lon], (lat, wrap(lon + i, 16)), kz)
    mark("s12_pump")
    pump("b", 3)
    pump("a", 1)
    pump("c", 3)
    pump("b", 4)
    mark("s15_pump")
    for c in in_late:
        c.wait()
    flags = 0.5 * jnp.sum(
        jnp.where(
            lax.broadcasted_iota(jnp.int32, (32, 32), 0) == lax.broadcasted_iota(jnp.int32, (32, 32), 1),
            jnp.broadcast_to(polar[...], (32, 32)), 0,
        ).astype(F32), axis=1, keepdims=True
    )
    lane256 = lax.broadcasted_iota(jnp.int32, (256, 128), 1)
    row256 = lax.broadcasted_iota(jnp.int32, (256, 128), 0)
    mine_at = jnp.sum(
        jnp.where(lane256 == number - lanes_at, tiles[...] - 64 * number, 0).astype(F32), axis=1, keepdims=True
    )
    spread = jnp.where(lane256 // 8 == lax.rem(row256, 16), mine_at, 0.0).astype(BF16)
    pick = (
        lax.broadcasted_iota(jnp.int32, (16, 256), 1) // 16 == lax.broadcasted_iota(jnp.int32, (16, 256), 0)
    ).astype(F32).astype(BF16)
    reg = dot(pick, spread).astype(jnp.int32)
    mark("s16_zwait")
    arrived(ybar.at[0:15], kz)
    mark("s17_surf")
    total = ybar[0]
    for i in range(1, 16):
        total = total + ybar[i]
    total = total * (1.0 / 2048.0)
    mean0 = jnp.concatenate([total] + [pltpu.roll(total, 128 - 8 * i, 1) for i in range(1, 4)], axis=0)

    def filtered(j, mean):
        v = aout[lax.rem(j, 8), j // 8]
        v = v + flags * (jnp.sum(jnp.where(lane == j, mean, 0.0), axis=1, keepdims=True) - v)
        aout[lax.rem(j, 8), j // 8] = v
        return v

    for t in range(8):
        surf[t] = filtered(t, mean0) * weight[...]

    mark("s18_pump")
    pump("c", 4)
    mark("s19_regions")

    sub8 = lax.broadcasted_iota(jnp.int32, (16, 128), 0)

    def regions(r, acc):
        lhs, rhs = [], [[], [], []]
        for h in range(2):
            i = 2 * r + h
            local = rl[pl.ds(i, 1), :]
            low = jnp.broadcast_to(local & 15, (16, 128))
            high = jnp.broadcast_to(local >> 4, (8, 128))
            lhs.append((low == sub8).astype(F32).astype(BF16))
            s = jnp.concatenate([surf[t, pl.ds(i, 1), :] for t in range(8)], axis=0)
            for n in range(3):
                piece = s.astype(BF16).astype(F32)
                s = s - piece
                rhs[n].append(
                    jnp.concatenate([jnp.where(high == a, piece, 0.0) for a in range(16)], axis=0).astype(BF16)
                )
        left = jnp.concatenate(lhs, axis=1)
        for n in range(3):
            acc = acc + dot_nt(left, jnp.concatenate(rhs[n], axis=1))
        return acc

    m = lax.fori_loop(0, 16, regions, jnp.zeros((16, 128), F32), unroll=4)
    for i in range(16):
        mbuf[i] = m[i:i + 1, :]
    xbuf[lon] = mbuf[lon]
    kx = take(xbuf.at[0:15])
    for i in range(1, 16):
        to = wrap(lon + i, 16)
        send(mbuf.at[to], xbuf.at[lon], (lat, to), kx)

    mark("s13_halo2b")
    pump("a", 2)
    pump("b", 5)
    pump("c", 5)
    pump("b", 6)
    sides2b = halo_wait(1, 1, 8, 64, k2b)
    mark("s14_step2b")
    sums = lax.fori_loop(8, 64, step_two(sides2b), none, unroll=UNROLL)
    lane16 = lax.broadcasted_iota(jnp.int32, (16, 128), 1)
    row16 = lax.broadcasted_iota(jnp.int32, (16, 128), 0)
    zbuf[lon] = jnp.where(lane16 < 64, sums[0:16], pltpu.roll(sums[16:32], 64, 1))
    kw = take(zbuf.at[0:15])
    for i in range(1, 16):
        send(zbuf.at[lon], zbuf.at[lon], (lat, wrap(lon + i, 16)), kw)
    mark("s20_pump")
    pump("c", 6)
    pump("a", 3)
    pump("b", 7)
    pump("c", 7)
    mark("s22_pump")
    mark("s23_xwait")
    arrived(xbuf.at[0:15], kx)
    mark("s24_turn")
    got = jnp.concatenate([xbuf[i] for i in range(16)], axis=0)
    turned = jnp.zeros((16, 128), F32)
    group = lane16 // 8
    for d in range(16):
        moved = got if d == 0 else pltpu.roll(pltpu.roll(got, 16 - d, 0), 8 * d, 1)
        turned = jnp.where(lax.rem(group - row16 + 16, 16) == d, moved, turned)
    for i in range(16):
        ybuf[i] = turned[i:i + 1, :]
    obuf[lat] = ybuf[lat]
    ky = take(obuf.at[0:15])
    for i in range(1, 16):
        to = wrap(lat + i, 16)
        send(ybuf.at[to], obuf.at[lat], (to, lon), ky)
    mark("s25_pump")
    pump("a", 4)
    pump("b", 8)
    pump("c", 8)
    pump("b", 9)
    mark("s21_rest")
    arrived(zbuf.at[0:15], kw)
    total = zbuf[0]
    for i in range(1, 16):
        total = total + zbuf[i]
    total = total * (1.0 / 2048.0)
    mean = jnp.concatenate([total, pltpu.roll(total, 64, 1)], axis=0)

    def rest(j, carry):
        filtered(j, mean)
        return carry

    lax.fori_loop(8, 64, rest, 0, unroll=UNROLL)
    out_field = load(aout, aout_h, 18)
    mark("s26_owait")
    pump("a", 5)
    pump("c", 9)
    pump("b", 10)
    pump("b", 11)
    arrived(obuf.at[0:15], ky)

    mark("s27_fresh")
    packed = jnp.zeros((8, 128), F32)
    for v in range(8):
        f = jnp.zeros((8, 128), F32)
        for a in range(16):
            f = f + jnp.where(reg[a:a + 1, :] == row8 + 8 * v, obuf[a], 0.0)
        for shift in (64, 32, 16, 8):
            f = f + pltpu.roll(f, shift, 1)
        packed = jnp.where(lane8 // 8 == v, f, packed)
    packed = packed.astype(BF16).astype(F32)
    fr[y, xl, z, xh] = (packed[0:4] + pltpu.roll(packed[4:8], 64, 1)).astype(BF16)
    kf = take(fr.at[0:3, 0, 0:5, 0])
    for i in range(1, 16):
        here = fr.at[y, xl, z, xh]
        send(here, here, (lat, wrap(lon + i, 16)), kf)
    mark("s28_pump")
    pump("a", 6)
    pump("c", 10)
    pump("b", 12)
    pump("b", 13)
    mark("s29_fwait")
    arrived(fr.at[0:3, 0, 0:5, 0], kf)
    kg = take(fr.at[:, :, 0:7])
    for i in range(1, 8):
        g = wrap(lat // 2 + i, 8)
        send(fr.at[y, xl], fr.at[y, xl], (g * 2 + core, lon), kg)
    mark("s30_pump")
    pump("a", 7)
    pump("c", 11)
    pump("b", 14)
    pltpu.make_async_copy(cmat.at[:, 0:64], cmat.at[:, 0:64], lsem.at[0]).wait()
    arrived(cmat.at[:, 0:64], k_cov)

    mark("s31_product")
    pacc[...] = jnp.zeros((2, 64, 512), F32)

    def product(g, carry):
        gy, gx = g // 2, lax.rem(g, 2)
        c = cmat[g]
        r0 = jnp.concatenate(
            [b0[gy, gx][:, :, 0:64].reshape(1024, 128), b1[gy, gx].reshape(1024, 128)], axis=1
        )
        left = dot(c, r0)
        pacc[0, :, 0:256] += left[0:64]
        pacc[1, :, 0:256] += left[64:128]
        tails = b0[gy, gx][:, :, 64:80].reshape(256, 128)
        pieces = []
        for q in range(4):
            sel = (
                lax.broadcasted_iota(jnp.int32, (128, 128), 0)
                == lax.broadcasted_iota(jnp.int32, (128, 128), 1) + 32 * q
            ).astype(F32).astype(BF16)
            pieces.append(dot(tails, sel).astype(BF16).reshape(16, 16, 128))
        last = jnp.concatenate(pieces, axis=1).reshape(1024, 128)
        right = dot(c, jnp.concatenate([b2[gy, gx].reshape(1024, 128), last], axis=1))
        pacc[0, :, 256:512] += right[0:64]
        pacc[1, :, 256:512] += right[64:128]
        return carry

    lax.fori_loop(0, 8, product, 0, unroll=2)
    kp = take(precv)
    send(pacc.at[1 - core], precv, other, kp)

    mark("s32_f2wait")
    arrived(fr.at[:, :, 0:7], kg)

    mark("s33_freshprod")

    def fresh_product(g, acc):
        f = fr[g // 2, lax.rem(g, 2)].reshape(16, 4, 128).astype(F32)
        f = jnp.concatenate([f, f], axis=1)
        lanes = (
            lax.broadcasted_iota(jnp.int32, (16, 8, 128), 2) // 8
            - lax.broadcasted_iota(jnp.int32, (16, 8, 128), 1) // 4 * 8
        )
        w = jnp.concatenate([jnp.where(lanes == v, f, 0.0) for v in range(8)], axis=1)
        return acc + dot(cmat[g], w.astype(BF16).reshape(1024, 128))

    added = lax.fori_loop(0, 8, fresh_product, jnp.zeros((128, 128), F32), unroll=4)
    for shift in (64, 32, 16, 8):
        added = added + pltpu.roll(added, shift, 1)
    aacc[0] = added[0:64]
    aacc[1] = added[64:128]
    mark("s34_exch")
    ka = take(arecv)
    send(aacc.at[1 - core], arecv, other, ka)
    arrived(precv, kp)
    arrived(arecv, ka)
    mark("s35_final")
    mine = aacc[core] + arecv[...]
    base = pacc[core] + precv[...]
    for n in range(4):
        week_of = (lax.broadcasted_iota(jnp.int32, (64, 128), 1) + 128 * n) // 8
        pre[:, 128 * n:128 * n + 128] = base[:, 128 * n:128 * n + 128] + jnp.where(
            week_of == jnp.broadcast_to(week[...], (64, 128)), mine, 0.0
        )
    out_pre = load(pre, pre_h, 19)
    for view, k in sends:
        remote(view, view, (lat, lon), k).wait_send()
    out_field.wait()
    out_pre.wait()
    mark("")


def finish(field, wide, aout, pre, held, block, trimmed, sem):
    reads = [pltpu.make_async_copy(field.at[t], held.at[t], sem.at[t]) for t in range(8)]
    small = pltpu.make_async_copy(wide, block, sem.at[8])
    small.start()
    for c in reads:
        c.start()
    small.wait()
    trimmed[...] = block[:, 0:416]
    writes = [pltpu.make_async_copy(trimmed, pre, sem.at[9])]
    writes[0].start()
    for t in range(8):
        reads[t].wait()
        c = pltpu.make_async_copy(held.at[t], aout.at[t], sem.at[10 + t])
        c.start()
        writes.append(c)
    for c in writes:
        c.wait()


COPIES = 64
UNROLL = 4
PROFILE = False


def shards(adjoint, transport, cell_weight, region_local, tile_regions, polar_rows, week_index, grad_in, covariance):
    hbm = pl.BlockSpec(memory_space=pl.ANY)
    aout, pre = pl.pallas_call(
        kernel,
        out_shape=(
            jax.ShapeDtypeStruct((8, 8, 32, 128), F32),
            jax.ShapeDtypeStruct((64, 512), F32),
        ),
        in_specs=[hbm] * 9,
        out_specs=(hbm, hbm),
        scratch_shapes=[
            pltpu.VMEM((8, 8, 32, 128), F32),
            pltpu.VMEM((6, 8, 32, 128), F32),
            pltpu.VMEM((32, 128), F32),
            pltpu.VMEM((32, 128), jnp.int32),
            pltpu.VMEM((256, 128), jnp.int32),
            pltpu.VMEM((1, 32), jnp.int32),
            pltpu.VMEM((1, 1), jnp.int32),
            pltpu.VMEM((64, 416), BF16),
            pltpu.VMEM((8, 8, 32, 128), F32),
            pltpu.VMEM((8, 32, 128), F32),
            pltpu.VMEM((4, 2, 8, 2, 80, 128), BF16),
            pltpu.VMEM((4, 2, 8, 2, 64, 128), BF16),
            pltpu.VMEM((4, 2, 8, 2, 64, 128), BF16),
            pltpu.VMEM((8, 128, 1024), BF16),
            pltpu.VMEM((4, 2, 8, 2, 4, 128), BF16),
            pltpu.VMEM((4, 32, 128), F32),
            pltpu.VMEM((2, 64, 128), F32),
            pltpu.VMEM((2, 64, 128), F32),
            pltpu.VMEM((4, 32, 128), F32),
            pltpu.VMEM((4, 32, 128), F32),
            pltpu.VMEM((2, 64, 128), F32),
            pltpu.VMEM((2, 64, 128), F32),
            pltpu.VMEM((16, 16, 128), F32),
            pltpu.VMEM((16, 8, 128), F32),
            pltpu.VMEM((16, 1, 128), F32),
            pltpu.VMEM((16, 1, 128), F32),
            pltpu.VMEM((16, 1, 128), F32),
            pltpu.VMEM((16, 1, 128), F32),
            pltpu.VMEM((2, 64, 512), F32),
            pltpu.VMEM((64, 512), F32),
            pltpu.VMEM((2, 64, 128), F32),
            pltpu.VMEM((64, 128), F32),
            pltpu.VMEM((8, 8, 32, 128), F32),
            pltpu.VMEM((64, 512), F32),
            pltpu.SemaphoreType.DMA((COPIES,)),
            pltpu.SemaphoreType.DMA((COPIES,)),
            pltpu.SemaphoreType.DMA((1,)),
            pltpu.SemaphoreType.DMA((20,)),
        ],
        compiler_params=pltpu.CompilerParams(
            collective_id=0, has_side_effects=True, vmem_limit_bytes=67043328
        ),
        name="window",
    )(
        adjoint, transport, cell_weight, region_local, tile_regions,
        polar_rows.reshape(1, 32), week_index.reshape(1, 1), grad_in, covariance,
    )
    return pl.pallas_call(
        finish,
        out_shape=(
            jax.ShapeDtypeStruct((8, 8, 32, 128), F32),
            jax.ShapeDtypeStruct((64, 416), F32),
        ),
        in_specs=[hbm] * 2,
        out_specs=(hbm, hbm),
        scratch_shapes=[
            pltpu.VMEM((8, 8, 32, 128), F32),
            pltpu.VMEM((64, 512), F32),
            pltpu.VMEM((64, 416), F32),
            pltpu.SemaphoreType.DMA((18,)),
        ],
        compiler_params=pltpu.CompilerParams(vmem_limit_bytes=67043328),
        name="finish",
    )(aout, pre)


def solution(mesh):
    both = ("lat", "lon")
    return jax.shard_map(
        shards,
        mesh=mesh,
        in_specs=(
            P(None, None, "lat", "lon"), P(None, None, "lat", "lon"), P("lat", "lon"), P("lat", "lon"),
            P(), P("lat"), P(), P(both, None), P(both, None),
        ),
        out_specs=(P(None, None, "lat", "lon"), P(both, None)),
        check_vma=False,
    )
```
